512 devices in a mesh: mem: 16 (over z_lo, y), tile: 32 (over z_hi, x, core).
Axes of the slice: x: 4, y: 8, z: 8 (z_hi: 4, z_lo: 2; z = z_hi * 2 + z_lo), core: 2. Of those that a mesh axis runs over, the one named last changes fastest.
Arguments:
- perturbations: bfloat16 [384, 3, 32, 32768], P('mem', None, None, 'tile'), may hold values from -6 to 6
- member_weight: float32 [384], P('mem'), may hold values from 0.3 to 3
- innovation: float32 [3, 32, 32768], P(None, 'mem', 'tile'), may hold values from -6 to 6
- obs_weight: float32 [3, 32], P(None, 'mem'), may hold values from 0.1 to 1
- static_var: float32 [3, 32, 32768], P(None, 'mem', 'tile'), may hold values from 0.1 to 1
- obs_mask: int32 [32768], P('tile'), may hold values 0 or 1
- kernel_x: float32 [32, 5], replicated, may hold values from 0.1 to 0.5
- kernel_y: float32 [32, 5], replicated, may hold values from 0.1 to 0.5
Outputs:
- analysis: float32 [3, 32, 32768], P(None, 'mem', 'tile')
The draws below stay inside these ranges and needn't reach their ends.
All inputs are finite; a program needn't handle non-finite values. No bound on the sum of `obs_mask` on one device may be relied on, other than what follows from the above.
Results may differ from the reference program's by a relative error of at most 0.0003.
Values sent between devices are 32-bit elements; how exact they have to be, the bound alone decides.
No kernel may reach another device: no remote copies, remote signals or barrier semaphores. Data moves between devices by JAX's collectives and lax.ppermute only.
A program may use at most 64 MiB of HBM per device.

```python
import math
import jax
import jax.numpy as jnp
from jax import lax

VARS = 3
LEVELS = 32
TILE_X = 32
TILE_Y = 32
GRID_Y = 4
STEPS = 2
MEMBER_COUNT_NUM = 384
NCOL = 32768
N_MEM = 16
N_TILE = 32


def touch_ends(result, own_key, smallest, top_value):
    place = [jax.random.randint(jax.random.fold_in(own_key, axis), (), 0, length) for axis, length in enumerate(result.shape)]
    main_axis = result.shape.index(max(result.shape))
    neighbour = place[:main_axis] + [(place[main_axis] + 1) % result.shape[main_axis]] + place[main_axis + 1:]
    return result.at[tuple(place)].set(smallest).at[tuple(neighbour)].set(top_value)


def levels(key, extent, shards, least, largest):
    factor_of, own = 1.0, jax.random.fold_in(key, 6)
    for dim, blocks in shards:
        steps = jnp.exp(jax.random.uniform(jax.random.fold_in(own, dim), (blocks,), jnp.float32, least / len(shards), largest / len(shards)))
        factor_of = factor_of * jnp.repeat(steps, extent[dim] // blocks).reshape([-1 if axis == dim else 1 for axis in range(len(extent))])
    return factor_of


def noise(key, extent, scale, most, pieces=(), kind=jnp.bfloat16):
    loudness = levels(key, extent, pieces, -0.22, 0.18) if pieces else 1.0
    drawn = jax.random.normal(key, extent, jnp.float32) * scale * loudness
    return jnp.minimum(jnp.maximum(drawn, -most), most).astype(kind)


def setup_inputs(seed: int = 0) -> dict:
    key_list = jax.random.split(jax.random.key(seed), 9)
    perturbations = noise(key_list[0], (MEMBER_COUNT_NUM, VARS, LEVELS, NCOL), 1.0, 6.0, ((0, 16), (3, 32)))
    member_weight = jnp.clip(jnp.exp(math.log(3.0) - 2.3025851 * jax.random.uniform(key_list[1], (MEMBER_COUNT_NUM,), jnp.float32) ** levels(key_list[1], (MEMBER_COUNT_NUM,), ((0, 16),), -0.2, 0.2)), 0.3, 3.0)
    innovation = noise(key_list[2], (VARS, LEVELS, NCOL), 1.0, 6.0, ((1, 16), (2, 32)), jnp.float32)
    obs_weight = jnp.clip(jnp.exp(math.log(1.0) - 2.3025851 * jax.random.uniform(key_list[3], (VARS, LEVELS), jnp.float32) ** levels(key_list[3], (VARS, LEVELS), ((1, 16),), -0.2, 0.2)), 0.1, 1.0)
    static_var = jnp.clip(jnp.exp(math.log(1.0) - 2.3025851 * jax.random.uniform(key_list[4], (VARS, LEVELS, NCOL), jnp.float32) ** levels(key_list[4], (VARS, LEVELS, NCOL), ((1, 16), (2, 32)), -0.2, 0.2)), 0.1, 1.0)
    obs_mask = touch_ends((jax.random.randint(key_list[5], (NCOL,), 0, 2) < 1).astype(jnp.int32), jax.random.fold_in(key_list[5], 1), 0, 1)
    kernel_x = jnp.clip(jnp.exp(jax.random.uniform(key_list[6], (LEVELS, 5), jnp.float32, math.log(0.1), math.log(0.5))), 0.1, 0.5)
    kernel_y = jnp.clip(jnp.exp(jax.random.uniform(key_list[7], (LEVELS, 5), jnp.float32, math.log(0.1), math.log(0.5))), 0.1, 0.5)
    return dict(perturbations=perturbations, member_weight=member_weight, innovation=innovation, obs_weight=obs_weight, static_var=static_var, obs_mask=obs_mask, kernel_x=kernel_x, kernel_y=kernel_y)


def interp_rows(fine_count, coarse_count):
    position = jnp.arange(fine_count, dtype=jnp.int32)
    lower_index = jnp.clip((position - 1) // 2, 0, coarse_count - 1)
    upper_index = jnp.clip((position - 1) // 2 + 1, 0, coarse_count - 1)
    fraction = jnp.where(position % 2 == 0, 0.75, 0.25).astype(jnp.float32)
    columns = jnp.arange(coarse_count, dtype=jnp.int32)
    lower_part = (lower_index[:, None] == columns[None, :]).astype(jnp.float32)
    upper_part = (upper_index[:, None] == columns[None, :]).astype(jnp.float32)
    return (1.0 - fraction)[:, None] * lower_part + fraction[:, None] * upper_part


def localize_all(member_projection, kernel_x, kernel_y, rows_x, rows_y):
    members = member_projection.shape[0]
    coarse_x = TILE_X // 2
    coarse_y = TILE_Y // 2
    grid_x = N_TILE // GRID_Y
    tiled = member_projection.reshape(members, LEVELS, N_TILE, TILE_X, TILE_Y)
    half = jnp.einsum("mltij,ia->mltaj", tiled, rows_x, precision=lax.Precision.HIGHEST)
    coarse = jnp.einsum("mltaj,jb->mltab", half, rows_y, precision=lax.Precision.HIGHEST)
    coarse = coarse.reshape(members, LEVELS, grid_x, GRID_Y, coarse_x, coarse_y)
    coarse = coarse.transpose(0, 1, 2, 4, 3, 5).reshape(members, LEVELS, grid_x * coarse_x, GRID_Y * coarse_y)
    summed_x = jnp.zeros_like(coarse)
    for offset in range(5):
        summed_x = summed_x + kernel_x[:, offset][None, :, None, None] * jnp.roll(coarse, 2 - offset, axis=2)
    padded = jnp.pad(summed_x, ((0, 0), (0, 0), (0, 0), (2, 2)))
    extent_y = GRID_Y * coarse_y
    summed_y = jnp.zeros_like(coarse)
    for offset in range(5):
        summed_y = summed_y + kernel_y[:, offset][None, :, None, None] * padded[:, :, :, offset:offset + extent_y]
    smoothed = summed_y.reshape(members, LEVELS, grid_x, coarse_x, GRID_Y, coarse_y)
    smoothed = smoothed.transpose(0, 1, 2, 4, 3, 5).reshape(members, LEVELS, N_TILE, coarse_x, coarse_y)
    half_fine = jnp.einsum("mltab,ia->mltib", smoothed, rows_x, precision=lax.Precision.HIGHEST)
    fine_resolution_state = jnp.einsum("mltib,jb->mltij", half_fine, rows_y, precision=lax.Precision.HIGHEST)
    return fine_resolution_state.reshape(members, LEVELS, NCOL)


def reference(perturbations, member_weight, innovation, obs_weight, static_var, obs_mask, kernel_x, kernel_y):
    rows_x = interp_rows(TILE_X, TILE_X // 2)
    rows_y = interp_rows(TILE_Y, TILE_Y // 2)
    observed = obs_mask.astype(jnp.float32)
    within_each_tile = MEMBER_COUNT_NUM // N_MEM
    blocks = perturbations.reshape(N_MEM, within_each_tile, VARS, LEVELS, NCOL)
    weight_blocks = member_weight.reshape(N_MEM, within_each_tile)

    def apply_ensemble(cost_gradient):
        def accumulate(summed, scanned):
            member_block, analysis_coefficients = scanned
            multi_tile_extent = member_block.astype(jnp.float32)
            member_projection = jnp.einsum("ohjr,hjr->ojr", multi_tile_extent, cost_gradient, precision=lax.Precision.HIGHEST)
            fine_resolution_state = localize_all(member_projection, kernel_x, kernel_y, rows_x, rows_y)
            addend_contribution = jnp.einsum("v,vhyp,vyp->hyp", analysis_coefficients / MEMBER_COUNT_NUM, multi_tile_extent, fine_resolution_state, precision=lax.Precision.HIGHEST)
            return summed + addend_contribution, None

        start = jnp.zeros((VARS, LEVELS, NCOL), jnp.float32)
        summed, _ = lax.scan(accumulate, start, (blocks, weight_blocks))
        return summed

    analysis = jnp.zeros((VARS, LEVELS, NCOL), jnp.float32)
    for repeat in range(STEPS):
        cost_gradient = observed[None, None, :] * obs_weight[:, :, None] * (analysis - innovation)
        increment = apply_ensemble(cost_gradient) + static_var * cost_gradient
        analysis = analysis - 0.5 * (analysis + increment)
    return analysis
```

```python
import functools
import math

import jax
import jax.numpy as jnp
import numpy as np
from jax import lax
from jax.experimental import pallas as pl
from jax.experimental.pallas import tpu as pltpu
from jax.sharding import PartitionSpec as P

VARS = 3
TILE_X = 32
TILE_Y = 32
GRID_Y = 4
STEPS = 2
CX = TILE_X // 2
CY = TILE_Y // 2
CELLS = CX * CY
COLS = TILE_X * TILE_Y
LANES = 128
CB = COLS // LANES
ROWS = VARS * CB
EXT = CX + 8
F32 = jnp.float32
BF16 = jnp.bfloat16


def interp_rows(fine_count):
    coarse_count = fine_count // 2
    rows = np.zeros((fine_count, coarse_count), np.float32)
    for i in range(fine_count):
        upper = 0.75 if i % 2 == 0 else 0.25
        low = (i - 1) // 2
        rows[i, min(max(low, 0), coarse_count - 1)] += 1.0 - upper
        rows[i, min(max(low + 1, 0), coarse_count - 1)] += upper
    return rows


def interp_matrix():
    rows_x, rows_y = interp_rows(TILE_X), interp_rows(TILE_Y)
    full = np.einsum("ia,jb->baij", rows_x, rows_y)
    return full.reshape(CELLS, COLS)


def vmem():
    return pl.BlockSpec(memory_space=pltpu.VMEM)


def grant(mib):
    return pltpu.CompilerParams(vmem_limit_bytes=mib * 1024 * 1024)


def split_terms(x):
    high = x.astype(BF16)
    return high, (x - high.astype(F32)).astype(BF16)


def split_levels_kernel(p_ref, _, o_ref, s_ref, *, own):
    members, _, levels, _ = p_ref.shape
    owners = levels // own
    start = pl.program_id(0) * members

    def one(k, carry):
        for v in range(VARS):
            for c in range(CB):
                s_ref[v * CB + c] = p_ref[k, v, :, c * LANES : (c + 1) * LANES].astype(F32)
        for v in range(VARS):
            for c in range(CB):
                for q in range(own):
                    o_ref[start + k, v, q, c] = s_ref[v * CB + c, pl.ds(q, owners, stride=own), :]
        return carry

    lax.fori_loop(0, members, one, 0)


def split_levels(perturbations, after, own):
    members, _, levels, _ = perturbations.shape
    step = math.gcd(members, 4)
    return pl.pallas_call(
        functools.partial(split_levels_kernel, own=own),
        grid=(members // step,),
        in_specs=[
            pl.BlockSpec((step, VARS, levels, COLS), lambda k: (k, 0, 0, 0)),
            pl.BlockSpec(memory_space=pl.ANY),
        ],
        out_specs=vmem(),
        out_shape=jax.ShapeDtypeStruct((members, VARS, own, CB, levels // own, LANES), F32),
        scratch_shapes=[pltpu.VMEM((VARS * CB, levels, LANES), F32)],
        compiler_params=grant(6),
        cost_estimate=pl.CostEstimate(flops=400_000_000, bytes_accessed=10_000_000, transcendentals=0),
        name="split_levels",
    )(perturbations, after)


def project_kernel(p_ref, g_ref, m_ref, c_ref, ylo_ref, yhi_ref, hi_ref, lo_ref, *, chunks):
    members, _, _, _, owners, _ = p_ref.shape
    tiles = members * owners // LANES
    for n, q in enumerate(chunks):
        for c in range(CB):
            lanes = slice(c * LANES, (c + 1) * LANES)
            grad = [
                g_ref[pl.ds((n * VARS + v) * CB + c, owners, stride=len(chunks) * ROWS), :]
                for v in range(VARS)
            ]

            def one(k, carry):
                acc = p_ref[k, 0, q, c] * grad[0]
                for v in range(1, VARS):
                    acc = acc + p_ref[k, v, q, c] * grad[v]
                high, low = split_terms(acc)
                at = pl.ds(pl.multiple_of(k * owners, owners), owners)
                hi_ref[at, lanes] = high
                lo_ref[at, lanes] = low
                return carry

            lax.fori_loop(0, members, one, 0, unroll=4)
        dims = (((1,), (1,)), ((), ()))
        coarse = lax.dot_general(m_ref[...], hi_ref[...], dims, preferred_element_type=F32)
        coarse = coarse + lax.dot_general(m_ref[...], lo_ref[...], dims, preferred_element_type=F32)
        for t in range(tiles):
            piece = coarse[:, t * LANES : (t + 1) * LANES]
            c_ref[n * tiles + t] = piece
            ylo_ref[n * tiles + t] = piece[: 2 * CX]
            yhi_ref[n * tiles + t] = piece[CELLS - 2 * CX :]


def project(split, gathered, matrix, chunks):
    members, _, _, _, owners, _ = split.shape
    tiles = len(chunks) * members * owners // LANES
    return pl.pallas_call(
        functools.partial(project_kernel, chunks=chunks),
        in_specs=[vmem(), vmem(), vmem()],
        out_specs=[vmem(), vmem(), vmem()],
        out_shape=[
            jax.ShapeDtypeStruct((tiles, CELLS, LANES), F32),
            jax.ShapeDtypeStruct((tiles, 2 * CX, LANES), F32),
            jax.ShapeDtypeStruct((tiles, 2 * CX, LANES), F32),
        ],
        scratch_shapes=[
            pltpu.VMEM((members * owners, COLS), BF16),
            pltpu.VMEM((members * owners, COLS), BF16),
        ],
        compiler_params=grant(8),
        name="project",
    )(split, gathered, matrix)


def smooth_y_kernel(c_ref, prev_ref, next_ref, k_ref, s_ref, xlo_ref, xhi_ref, *, chunks):
    tiles = c_ref.shape[0]
    for t in range(tiles):
        q = chunks[t * len(chunks) // tiles]
        coef = [k_ref[d : d + 1, q * LANES : (q + 1) * LANES] for d in range(5)]

        def rows(b):
            if b < 0:
                return prev_ref[t, (b + 2) * CX : (b + 3) * CX, :]
            if b >= CY:
                return next_ref[t, (b - CY) * CX : (b - CY + 1) * CX, :]
            return c_ref[t, b * CX : (b + 1) * CX, :]

        for b in range(CY):
            acc = coef[0] * rows(b - 2)
            for d in range(1, 5):
                acc = acc + coef[d] * rows(b + d - 2)
            s_ref[t, b * CX : (b + 1) * CX, :] = acc
        for j in range(2):
            xlo_ref[t, j * CY : (j + 1) * CY, :] = s_ref[t, pl.ds(j, CY, stride=CX), :]
            xhi_ref[t, j * CY : (j + 1) * CY, :] = s_ref[t, pl.ds(CX - 2 + j, CY, stride=CX), :]


def smooth_y(coarse, from_prev, from_next, coefs, chunks):
    tiles = coarse.shape[0]
    return pl.pallas_call(
        functools.partial(smooth_y_kernel, chunks=chunks),
        in_specs=[vmem()] * 4,
        out_specs=[vmem()] * 3,
        out_shape=[
            jax.ShapeDtypeStruct((tiles, CELLS, LANES), F32),
            jax.ShapeDtypeStruct((tiles, 2 * CY, LANES), F32),
            jax.ShapeDtypeStruct((tiles, 2 * CY, LANES), F32),
        ],
        compiler_params=grant(2),
        name="smooth_y",
    )(coarse, from_prev, from_next, coefs)


def increment_kernel(p_ref, s_ref, prev_ref, next_ref, k_ref, w_ref, m_ref, o_ref, e_ref, hi_ref, lo_ref, f_ref, *, chunks):
    members, _, _, _, owners, _ = p_ref.shape
    tiles = members * owners // LANES
    for n, q in enumerate(chunks):
        for t in range(tiles):
            at = n * tiles + t
            for b in range(CY):
                e_ref[b * EXT + 8 : b * EXT + 8 + CX, :] = s_ref[at, b * CX : (b + 1) * CX, :]
            for j in range(2):
                e_ref[pl.ds(6 + j, CY, stride=EXT), :] = prev_ref[at, j * CY : (j + 1) * CY, :]
                e_ref[pl.ds(8 + CX + j, CY, stride=EXT), :] = next_ref[at, j * CY : (j + 1) * CY, :]
            scale = w_ref[:, t * LANES : (t + 1) * LANES]
            coef = [k_ref[d : d + 1, q * LANES : (q + 1) * LANES] * scale for d in range(5)]
            for b in range(CY):
                acc = coef[0] * e_ref[b * EXT + 6 : b * EXT + 6 + CX, :]
                for d in range(1, 5):
                    acc = acc + coef[d] * e_ref[b * EXT + 6 + d : b * EXT + 6 + d + CX, :]
                high, low = split_terms(acc)
                hi_ref[b * CX : (b + 1) * CX, t * LANES : (t + 1) * LANES] = high
                lo_ref[b * CX : (b + 1) * CX, t * LANES : (t + 1) * LANES] = low
        dims = (((0,), (0,)), ((), ()))
        fine = lax.dot_general(hi_ref[...], m_ref[...], dims, preferred_element_type=F32)
        f_ref[...] = fine + lax.dot_general(lo_ref[...], m_ref[...], dims, preferred_element_type=F32)
        for c in range(CB):
            lanes = slice(c * LANES, (c + 1) * LANES)

            def one(k, acc):
                at = pl.ds(pl.multiple_of(k * owners, owners), owners)
                local = f_ref[at, lanes]
                return tuple(acc[v] + p_ref[k, v, q, c] * local for v in range(VARS))

            zero = jnp.zeros((owners, LANES), F32)
            acc = lax.fori_loop(0, members, one, (zero,) * VARS, unroll=4)
            for v in range(VARS):
                o_ref[pl.ds((n * VARS + v) * CB + c, owners, stride=len(chunks) * ROWS), :] = acc[v]


def increment(split, smoothed, from_prev, from_next, coefs, scale, matrix, chunks):
    members, _, _, _, owners, _ = split.shape
    return pl.pallas_call(
        functools.partial(increment_kernel, chunks=chunks),
        in_specs=[vmem()] * 7,
        out_specs=vmem(),
        out_shape=jax.ShapeDtypeStruct((owners * len(chunks) * ROWS, LANES), F32),
        scratch_shapes=[
            pltpu.VMEM((CY * EXT + 8, LANES), F32),
            pltpu.VMEM((CELLS, members * owners), BF16),
            pltpu.VMEM((CELLS, members * owners), BF16),
            pltpu.VMEM((members * owners, COLS), F32),
        ],
        compiler_params=grant(8),
        name="increment",
    )(split, smoothed, from_prev, from_next, coefs, scale, matrix)


def prepare_kernel(
    inn_ref, sv_ref, mask_ref, w_ref, kx_ref, ky_ref, mw_ref, level_ref, member_ref,
    innov_ref, static_ref, weight_ref, grad_ref, send_ref, cx_ref, cy_ref, scale_ref,
    *, norm,
):
    own = inn_ref.shape[1]
    for q in range(own):
        for v in range(VARS):
            for c in range(CB):
                row = (q * VARS + v) * CB + c
                lanes = slice(c * LANES, (c + 1) * LANES)
                innov_ref[row : row + 1, :] = inn_ref[v, q : q + 1, lanes]
                static_ref[row : row + 1, :] = sv_ref[v, q : q + 1, lanes]
            rows = slice((q * VARS + v) * CB, (q * VARS + v + 1) * CB)
            weight_ref[rows, :] = mask_ref[...].astype(F32) * w_ref[v, q]
    grad = weight_ref[...] * (0.0 - innov_ref[...])
    grad_ref[...] = grad
    rows = grad.shape[0]
    for d in range(send_ref.shape[0] // rows):
        send_ref[d * rows : (d + 1) * rows, :] = grad
    exact = lax.Precision.HIGHEST
    cx_ref[...] = jnp.dot(kx_ref[...], level_ref[...], precision=exact, preferred_element_type=F32)
    cy_ref[...] = jnp.dot(ky_ref[...], level_ref[...], precision=exact, preferred_element_type=F32)
    scale = jnp.dot(mw_ref[...], member_ref[...], precision=exact, preferred_element_type=F32)
    scale_ref[...] = scale / norm


def prepare(innovation, static_var, obs_mask, obs_weight, kernel_x, kernel_y, member_weight, size):
    _, own, _ = innovation.shape
    members, levels = member_weight.shape[0], kernel_x.shape[0]
    rows = own * ROWS
    lane = np.arange(own * LANES)
    level = own * (lane % LANES % size) + lane // LANES
    pick_level = (np.arange(levels)[:, None] == level[None, :]).astype(np.float32)
    pick_member = (np.arange(members)[:, None] == np.arange(members * size)[None, :] // size).astype(np.float32)
    flat = [jax.ShapeDtypeStruct((rows, LANES), F32)] * 4
    coefs = [jax.ShapeDtypeStruct((5, own * LANES), F32)] * 2
    return pl.pallas_call(
        functools.partial(prepare_kernel, norm=float(size * members)),
        in_specs=[vmem()] * 3 + [pl.BlockSpec(memory_space=pltpu.SMEM)] + [vmem()] * 5,
        out_specs=[vmem()] * 8,
        out_shape=flat
        + [jax.ShapeDtypeStruct((size * rows, LANES), F32)]
        + coefs
        + [jax.ShapeDtypeStruct((1, members * size), F32)],
        compiler_params=grant(2),
        name="prepare",
    )(
        innovation, static_var, obs_mask.reshape(CB, LANES), obs_weight, kernel_x.T, kernel_y.T,
        member_weight.reshape(1, -1), jnp.asarray(pick_level), jnp.asarray(pick_member),
    )


def update_kernel(r_ref, *refs, size, last):
    ins, outs = (refs[:3], refs[3:]) if last else (refs[:4], refs[4:])
    rows = ins[0].shape[0]
    total = r_ref[:rows, :]
    for d in range(1, size):
        total = total + r_ref[d * rows : (d + 1) * rows, :]
    if last:
        a_ref, g_ref, sv_ref = ins
        analysis = a_ref[...]
    else:
        g_ref, sv_ref, w_ref, inn_ref = ins
        analysis = jnp.zeros_like(total)
    inc = total + sv_ref[...] * g_ref[...]
    analysis = analysis - 0.5 * (analysis + inc)
    if last:
        own = rows // ROWS
        for q in range(own):
            for v in range(VARS):
                for c in range(CB):
                    row = (q * VARS + v) * CB + c
                    outs[0][v, q : q + 1, c * LANES : (c + 1) * LANES] = analysis[row : row + 1, :]
        return
    grad = w_ref[...] * (analysis - inn_ref[...])
    outs[0][...] = analysis
    outs[1][...] = grad
    for d in range(size):
        outs[2][d * rows : (d + 1) * rows, :] = grad


def update(received, args, size, last):
    rows = received.shape[0] // size
    flat = jax.ShapeDtypeStruct((rows, LANES), F32)
    if last:
        shapes = [jax.ShapeDtypeStruct((VARS, rows // ROWS, COLS), F32)]
    else:
        shapes = [flat, flat, jax.ShapeDtypeStruct((size * rows, LANES), F32)]
    return pl.pallas_call(
        functools.partial(update_kernel, size=size, last=last),
        in_specs=[vmem()] * (1 + len(args)),
        out_specs=[vmem()] * len(shapes),
        out_shape=shapes,
        compiler_params=grant(2),
        name="update",
    )(received, *args)


def exchange(x, size):
    blocks = x.reshape(size, -1, LANES)
    return lax.all_to_all(blocks, "mem", 0, 0, tiled=True).reshape(x.shape)


def along_x(x, by):
    size = lax.axis_size("tile")
    return lax.ppermute(x, "tile", [(i, (i + by * GRID_Y) % size) for i in range(size)])


def along_y(x, by):
    size = lax.axis_size("tile")
    return lax.ppermute(x, "tile", [(i, i + by) for i in range(size) if 0 <= i % GRID_Y + by < GRID_Y])


def body(perturbations, member_weight, innovation, obs_weight, static_var, obs_mask, kernel_x, kernel_y):
    size = lax.axis_size("mem")
    own = perturbations.shape[2] // size
    chunks = tuple(range(own))
    matrix = jnp.asarray(interp_matrix(), BF16)
    innov, static, weight, gradient, to_send, coef_x, coef_y, scale = prepare(
        innovation, static_var, obs_mask, obs_weight, kernel_x, kernel_y, member_weight, size
    )
    analysis = split = None
    for step in range(STEPS):
        gathered = exchange(to_send, size)
        if split is None:
            split = split_levels(perturbations, gathered, own)
        coarse, ylo, yhi = project(split, gathered, matrix, chunks)
        from_prev, from_next = along_y(yhi, 1), along_y(ylo, -1)
        smoothed, xlo, xhi = smooth_y(coarse, from_prev, from_next, coef_y, chunks)
        from_prev, from_next = along_x(xhi, 1), along_x(xlo, -1)
        partial = increment(split, smoothed, from_prev, from_next, coef_x, scale, matrix, chunks)
        received = exchange(partial, size)
        if step == STEPS - 1:
            return update(received, (analysis, gradient, static), size, True)[0]
        analysis, gradient, to_send = update(received, (gradient, static, weight, innov), size, False)


def solution(mesh):
    placed = (
        P("mem", None, None, "tile"),
        P("mem"),
        P(None, "mem", "tile"),
        P(None, "mem"),
        P(None, "mem", "tile"),
        P("tile"),
        P(),
        P(),
    )
    return jax.shard_map(
        body, mesh=mesh, in_specs=placed, out_specs=P(None, "mem", "tile"), check_vma=False
    )
```

```python
import functools
import math

import jax
import jax.numpy as jnp
import numpy as np
from jax import lax
from jax.experimental import pallas as pl
from jax.experimental.pallas import tpu as pltpu
from jax.sharding import PartitionSpec as P


VARS = 3
TILE_X = 32
TILE_Y = 32
GRID_Y = 4
STEPS = 2
CX = TILE_X // 2
CY = TILE_Y // 2
CELLS = CX * CY
COLS = TILE_X * TILE_Y
LANES = 128
CB = COLS // LANES
ROWS = VARS * CB
EXT = CX + 8
F32 = jnp.float32
BF16 = jnp.bfloat16


def interp_rows(fine_count):
    coarse_count = fine_count // 2
    rows = np.zeros((fine_count, coarse_count), np.float32)
    for i in range(fine_count):
        upper = 0.75 if i % 2 == 0 else 0.25
        low = (i - 1) // 2
        rows[i, min(max(low, 0), coarse_count - 1)] += 1.0 - upper
        rows[i, min(max(low + 1, 0), coarse_count - 1)] += upper
    return rows


def interp_matrix():
    rows_x, rows_y = interp_rows(TILE_X), interp_rows(TILE_Y)
    full = np.einsum("ia,jb->baij", rows_x, rows_y)
    return full.reshape(CELLS, COLS)


def vmem():
    return pl.BlockSpec(memory_space=pltpu.VMEM)


def grant(mib):
    return pltpu.CompilerParams(vmem_limit_bytes=mib * 1024 * 1024)


def split_terms(x):
    high = x.astype(BF16)
    return high, (x - high.astype(F32)).astype(BF16)


def in_hbm(x):
    return pltpu.with_memory_space_constraint(x, pltpu.HBM)


def whole(x, space=pltpu.VMEM):
    zeros = (0,) * x.ndim
    return pl.BlockSpec(x.shape, lambda k: zeros, memory_space=space)


def picked(rows, cols, wanted):
    row = lax.broadcasted_iota(jnp.int32, (rows, cols), 0)
    col = lax.broadcasted_iota(jnp.int32, (rows, cols), 1)
    return jnp.where(row == wanted(col), 1.0, 0.0).astype(F32)


def opening_kernel(
    p_ref, inn_ref, sv_ref, mask_ref, w_ref, kx_ref, ky_ref, mw_ref, m_ref,
    split_ref, matrix_ref, innov_ref, static_ref, weight_ref, grad_ref, send_ref, cx_ref, cy_ref, scale_ref,
    s_ref, *, size,
):
    own = inn_ref.shape[1]
    shift = size.bit_length() - 1
    block, _, levels, _ = p_ref.shape
    members = mw_ref.shape[1]
    start = pl.program_id(0) * block

    @pl.when(pl.program_id(0) == 0)
    def _():
        for q in range(own):
            for v in range(VARS):
                for c in range(CB):
                    row = (q * VARS + v) * CB + c
                    lanes = slice(c * LANES, (c + 1) * LANES)
                    innov_ref[row : row + 1, :] = inn_ref[v, q : q + 1, lanes]
                    static_ref[row : row + 1, :] = sv_ref[v, q : q + 1, lanes]
                rows = slice((q * VARS + v) * CB, (q * VARS + v + 1) * CB)
                weight_ref[rows, :] = mask_ref[...].astype(F32) * w_ref[q, v]
        grad = weight_ref[...] * (0.0 - innov_ref[...])
        grad_ref[...] = grad
        rows = grad.shape[0]
        for d in range(size):
            send_ref[d * rows : (d + 1) * rows, :] = grad
        exact = lax.Precision.HIGHEST
        lane_bits = LANES.bit_length() - 1
        level = picked(levels, own * LANES, lambda c: own * (c & (size - 1)) + (c >> lane_bits))
        member = picked(members, members * size, lambda c: c >> shift)
        cx_ref[...] = jnp.dot(kx_ref[...], level, precision=exact, preferred_element_type=F32)
        cy_ref[...] = jnp.dot(ky_ref[...], level, precision=exact, preferred_element_type=F32)
        scale = jnp.dot(mw_ref[...], member, precision=exact, preferred_element_type=F32)
        scale_ref[...] = scale / float(size * members)
        matrix_ref[...] = m_ref[...]

    def one(k, carry):
        for v in range(VARS):
            for c in range(CB):
                s_ref[v * CB + c] = p_ref[k, v, :, c * LANES : (c + 1) * LANES].astype(F32)
        for v in range(VARS):
            for c in range(CB):
                for q in range(own):
                    split_ref[start + k, v, q, c] = s_ref[v * CB + c, pl.ds(q, size, stride=own), :]
        return carry

    lax.fori_loop(0, block, one, 0)


def opening(perturbations, innovation, static_var, obs_mask, obs_weight, kernel_x, kernel_y, member_weight, size):
    members, _, levels, _ = perturbations.shape
    own = levels // size
    block = math.gcd(members, 4)
    rows = own * ROWS
    small = [
        innovation, static_var, obs_mask.reshape(CB, LANES), obs_weight.T,
        kernel_x.T, kernel_y.T, member_weight.reshape(1, -1), jnp.asarray(interp_matrix(), BF16),
    ]
    specs = [whole(x, pltpu.SMEM if n == 3 else pltpu.VMEM) for n, x in enumerate(small)]
    shapes = (
        [jax.ShapeDtypeStruct((members, VARS, own, CB, size, LANES), F32), jax.ShapeDtypeStruct((CELLS, COLS), BF16)]
        + [jax.ShapeDtypeStruct((rows, LANES), F32)] * 4
        + [jax.ShapeDtypeStruct((size * rows, LANES), F32)]
        + [jax.ShapeDtypeStruct((5, own * LANES), F32)] * 2
        + [jax.ShapeDtypeStruct((1, members * size), F32)]
    )
    return pl.pallas_call(
        functools.partial(opening_kernel, size=size),
        grid=(members // block,),
        in_specs=[pl.BlockSpec((block, VARS, levels, COLS), lambda k: (k, 0, 0, 0))] + specs,
        out_specs=[vmem()] * len(shapes),
        out_shape=shapes,
        scratch_shapes=[pltpu.VMEM((VARS * CB, levels, LANES), F32)],
        compiler_params=grant(6),
        name="opening",
    )(*[in_hbm(x) for x in [perturbations] + small])


def project_kernel(p_ref, g_ref, m_ref, c_ref, near_ref, far_ref, hi_ref, lo_ref, *, chunks):
    odd = lax.axis_index("tile") % GRID_Y % 2
    edge = CELLS - 2 * CX
    near_at = pl.ds(pl.multiple_of((1 - odd) * edge, 8), 2 * CX)
    far_at = pl.ds(pl.multiple_of(odd * edge, 8), 2 * CX)
    members, _, _, _, owners, _ = p_ref.shape
    tiles = members * owners // LANES
    for n, q in enumerate(chunks):
        for c in range(CB):
            lanes = slice(c * LANES, (c + 1) * LANES)
            grad = [
                g_ref[pl.ds((n * VARS + v) * CB + c, owners, stride=len(chunks) * ROWS), :]
                for v in range(VARS)
            ]

            def one(k, carry):
                acc = p_ref[k, 0, q, c] * grad[0]
                for v in range(1, VARS):
                    acc = acc + p_ref[k, v, q, c] * grad[v]
                high, low = split_terms(acc)
                at = pl.ds(pl.multiple_of(k * owners, owners), owners)
                hi_ref[at, lanes] = high
                lo_ref[at, lanes] = low
                return carry

            lax.fori_loop(0, members, one, 0, unroll=4)
        dims = (((1,), (1,)), ((), ()))
        coarse = lax.dot_general(m_ref[...], hi_ref[...], dims, preferred_element_type=F32)
        coarse = coarse + lax.dot_general(m_ref[...], lo_ref[...], dims, preferred_element_type=F32)
        for t in range(tiles):
            piece = coarse[:, t * LANES : (t + 1) * LANES]
            c_ref[n * tiles + t] = piece
        for t in range(n * tiles, (n + 1) * tiles):
            near_ref[t] = c_ref[t, near_at, :]
            far_ref[t] = c_ref[t, far_at, :]


def project(split, gathered, matrix, chunks):
    members, _, _, _, owners, _ = split.shape
    tiles = len(chunks) * members * owners // LANES
    return pl.pallas_call(
        functools.partial(project_kernel, chunks=chunks),
        in_specs=[vmem(), vmem(), vmem()],
        out_specs=[vmem(), vmem(), vmem()],
        out_shape=[
            jax.ShapeDtypeStruct((tiles, CELLS, LANES), F32),
            jax.ShapeDtypeStruct((tiles, 2 * CX, LANES), F32),
            jax.ShapeDtypeStruct((tiles, 2 * CX, LANES), F32),
        ],
        scratch_shapes=[
            pltpu.VMEM((members * owners, COLS), BF16),
            pltpu.VMEM((members * owners, COLS), BF16),
        ],
        compiler_params=grant(8),
        name="project",
    )(split, gathered, matrix)


def sides(near, far, odd):
    return jnp.where(odd, near, far), jnp.where(odd, far, near)


def smooth_y_kernel(c_ref, near_ref, far_ref, k_ref, s_ref, xnear_ref, xfar_ref, *, chunks):
    tile = lax.axis_index("tile")
    odd_y, odd_x = tile % GRID_Y % 2 == 1, tile // GRID_Y % 2 == 1
    tiles = c_ref.shape[0]
    for t in range(tiles):
        q = chunks[t * len(chunks) // tiles]
        coef = [k_ref[d : d + 1, q * LANES : (q + 1) * LANES] for d in range(5)]
        before, after = sides(near_ref[t], far_ref[t], odd_y)

        def rows(b):
            if b < 0:
                return before[(b + 2) * CX : (b + 3) * CX, :]
            if b >= CY:
                return after[(b - CY) * CX : (b - CY + 1) * CX, :]
            return c_ref[t, b * CX : (b + 1) * CX, :]

        for b in range(CY):
            acc = coef[0] * rows(b - 2)
            for d in range(1, 5):
                acc = acc + coef[d] * rows(b + d - 2)
            s_ref[t, b * CX : (b + 1) * CX, :] = acc
        for j in range(2):
            low = s_ref[t, pl.ds(j, CY, stride=CX), :]
            high = s_ref[t, pl.ds(CX - 2 + j, CY, stride=CX), :]
            xnear_ref[t, j * CY : (j + 1) * CY, :], xfar_ref[t, j * CY : (j + 1) * CY, :] = sides(low, high, odd_x)


def smooth_y(coarse, near, far, coefs, chunks):
    tiles = coarse.shape[0]
    return pl.pallas_call(
        functools.partial(smooth_y_kernel, chunks=chunks),
        in_specs=[vmem()] * 4,
        out_specs=[vmem()] * 3,
        out_shape=[
            jax.ShapeDtypeStruct((tiles, CELLS, LANES), F32),
            jax.ShapeDtypeStruct((tiles, 2 * CY, LANES), F32),
            jax.ShapeDtypeStruct((tiles, 2 * CY, LANES), F32),
        ],
        compiler_params=grant(2),
        name="smooth_y",
    )(coarse, near, far, coefs)


def increment_kernel(p_ref, s_ref, near_ref, far_ref, k_ref, w_ref, m_ref, o_ref, e_ref, hi_ref, lo_ref, f_ref, *, chunks):
    odd_x = lax.axis_index("tile") // GRID_Y % 2 == 1
    members, _, _, _, owners, _ = p_ref.shape
    tiles = members * owners // LANES
    for n, q in enumerate(chunks):
        for t in range(tiles):
            at = n * tiles + t
            for b in range(CY):
                e_ref[b * EXT + 8 : b * EXT + 8 + CX, :] = s_ref[at, b * CX : (b + 1) * CX, :]
            before, after = sides(near_ref[at], far_ref[at], odd_x)
            for j in range(2):
                e_ref[pl.ds(6 + j, CY, stride=EXT), :] = before[j * CY : (j + 1) * CY, :]
                e_ref[pl.ds(8 + CX + j, CY, stride=EXT), :] = after[j * CY : (j + 1) * CY, :]
            scale = w_ref[:, t * LANES : (t + 1) * LANES]
            coef = [k_ref[d : d + 1, q * LANES : (q + 1) * LANES] * scale for d in range(5)]
            for b in range(CY):
                acc = coef[0] * e_ref[b * EXT + 6 : b * EXT + 6 + CX, :]
                for d in range(1, 5):
                    acc = acc + coef[d] * e_ref[b * EXT + 6 + d : b * EXT + 6 + d + CX, :]
                high, low = split_terms(acc)
                hi_ref[b * CX : (b + 1) * CX, t * LANES : (t + 1) * LANES] = high
                lo_ref[b * CX : (b + 1) * CX, t * LANES : (t + 1) * LANES] = low
        dims = (((0,), (0,)), ((), ()))
        fine = lax.dot_general(hi_ref[...], m_ref[...], dims, preferred_element_type=F32)
        f_ref[...] = fine + lax.dot_general(lo_ref[...], m_ref[...], dims, preferred_element_type=F32)
        for c in range(CB):
            lanes = slice(c * LANES, (c + 1) * LANES)

            def one(k, acc):
                at = pl.ds(pl.multiple_of(k * owners, owners), owners)
                local = f_ref[at, lanes]
                return tuple(acc[v] + p_ref[k, v, q, c] * local for v in range(VARS))

            zero = jnp.zeros((owners, LANES), F32)
            acc = lax.fori_loop(0, members, one, (zero,) * VARS, unroll=4)
            for v in range(VARS):
                o_ref[pl.ds((n * VARS + v) * CB + c, owners, stride=len(chunks) * ROWS), :] = acc[v]


def increment(split, smoothed, near, far, coefs, scale, matrix, chunks):
    members, _, _, _, owners, _ = split.shape
    return pl.pallas_call(
        functools.partial(increment_kernel, chunks=chunks),
        in_specs=[vmem()] * 7,
        out_specs=vmem(),
        out_shape=jax.ShapeDtypeStruct((owners * len(chunks) * ROWS, LANES), F32),
        scratch_shapes=[
            pltpu.VMEM((CY * EXT + 8, LANES), F32),
            pltpu.VMEM((CELLS, members * owners), BF16),
            pltpu.VMEM((CELLS, members * owners), BF16),
            pltpu.VMEM((members * owners, COLS), F32),
        ],
        compiler_params=grant(8),
        name="increment",
    )(split, smoothed, near, far, coefs, scale, matrix)


def update_kernel(r_ref, *refs, size, last):
    ins, outs = (refs[:3], refs[3:]) if last else (refs[:4], refs[4:])
    rows = ins[0].shape[0]
    total = r_ref[:rows, :]
    for d in range(1, size):
        total = total + r_ref[d * rows : (d + 1) * rows, :]
    if last:
        a_ref, g_ref, sv_ref = ins
        analysis = a_ref[...]
    else:
        g_ref, sv_ref, w_ref, inn_ref = ins
        analysis = jnp.zeros_like(total)
    inc = total + sv_ref[...] * g_ref[...]
    analysis = analysis - 0.5 * (analysis + inc)
    if last:
        own = rows // ROWS
        for q in range(own):
            for v in range(VARS):
                for c in range(CB):
                    row = (q * VARS + v) * CB + c
                    outs[0][v, q : q + 1, c * LANES : (c + 1) * LANES] = analysis[row : row + 1, :]
        return
    grad = w_ref[...] * (analysis - inn_ref[...])
    outs[0][...] = analysis
    outs[1][...] = grad
    for d in range(size):
        outs[2][d * rows : (d + 1) * rows, :] = grad


def update(received, args, size, last):
    rows = received.shape[0] // size
    flat = jax.ShapeDtypeStruct((rows, LANES), F32)
    if last:
        shapes = [jax.ShapeDtypeStruct((VARS, rows // ROWS, COLS), F32)]
    else:
        shapes = [flat, flat, jax.ShapeDtypeStruct((size * rows, LANES), F32)]
    return pl.pallas_call(
        functools.partial(update_kernel, size=size, last=last),
        in_specs=[vmem()] * (1 + len(args)),
        out_specs=[vmem()] * len(shapes),
        out_shape=shapes,
        compiler_params=grant(2),
        name="update",
    )(received, *args)


def exchange(x, size):
    blocks = x.reshape(size, -1, LANES)
    return lax.all_to_all(blocks, "mem", 0, 0, tiled=True).reshape(x.shape)


def swapped(near, far, stride, places, periodic):
    def pairs(is_near):
        out = []
        for i in range(lax.axis_size("tile")):
            place = i // stride % places
            to = place + (1 if (place % 2 == 0) == is_near else -1)
            if periodic or 0 <= to < places:
                out.append((i, i + (to % places - place) * stride))
        return out

    from_far = lax.ppermute(far, "tile", pairs(False))
    from_near = lax.ppermute(near, "tile", pairs(True))
    return from_near, from_far


def body(perturbations, member_weight, innovation, obs_weight, static_var, obs_mask, kernel_x, kernel_y):
    size = lax.axis_size("mem")
    grid_x = lax.axis_size("tile") // GRID_Y
    chunks = tuple(range(perturbations.shape[2] // size))
    split, matrix, innov, static, weight, gradient, to_send, coef_x, coef_y, scale = opening(
        perturbations, innovation, static_var, obs_mask, obs_weight, kernel_x, kernel_y, member_weight, size
    )
    analysis = None
    for step in range(STEPS):
        gathered = exchange(to_send, size)
        coarse, near, far = project(split, gathered, matrix, chunks)
        near, far = swapped(near, far, 1, GRID_Y, False)
        smoothed, near, far = smooth_y(coarse, near, far, coef_y, chunks)
        near, far = swapped(near, far, GRID_Y, grid_x, True)
        partial = increment(split, smoothed, near, far, coef_x, scale, matrix, chunks)
        received = exchange(partial, size)
        if step == STEPS - 1:
            return update(received, (analysis, gradient, static), size, True)[0]
        analysis, gradient, to_send = update(received, (gradient, static, weight, innov), size, False)


def solution(mesh):
    placed = (
        P("mem", None, None, "tile"),
        P("mem"),
        P(None, "mem", "tile"),
        P(None, "mem"),
        P(None, "mem", "tile"),
        P("tile"),
        P(),
        P(),
    )
    return jax.shard_map(
        body, mesh=mesh, in_specs=placed, out_specs=P(None, "mem", "tile"), check_vma=False
    )
```

```python
import functools
import math

import jax
import jax.numpy as jnp
import numpy as np
from jax import lax
from jax.experimental import pallas as pl
from jax.experimental.pallas import tpu as pltpu
from jax.sharding import PartitionSpec as P


VARS = 3
TILE_X = 32
TILE_Y = 32
GRID_Y = 4
STEPS = 2
CX = TILE_X // 2
CY = TILE_Y // 2
CELLS = CX * CY
COLS = TILE_X * TILE_Y
LANES = 128
CB = COLS // LANES
ROWS = VARS * CB
EXT = CX + 8
F32 = jnp.float32
BF16 = jnp.bfloat16


def interp_rows(fine_count):
    coarse_count = fine_count // 2
    rows = np.zeros((fine_count, coarse_count), np.float32)
    for i in range(fine_count):
        upper = 0.75 if i % 2 == 0 else 0.25
        low = (i - 1) // 2
        rows[i, min(max(low, 0), coarse_count - 1)] += 1.0 - upper
        rows[i, min(max(low + 1, 0), coarse_count - 1)] += upper
    return rows


def interp_matrix():
    rows_x, rows_y = interp_rows(TILE_X), interp_rows(TILE_Y)
    full = np.einsum("ia,jb->baij", rows_x, rows_y)
    return full.reshape(CELLS, COLS)


def vmem():
    return pl.BlockSpec(memory_space=pltpu.VMEM)


def grant(mib):
    return pltpu.CompilerParams(vmem_limit_bytes=mib * 1024 * 1024)


def split_terms(x):
    high = x.astype(BF16)
    return high, (x - high.astype(F32)).astype(BF16)


def in_hbm(x):
    return pltpu.with_memory_space_constraint(x, pltpu.HBM)


def whole(x, space=pltpu.VMEM):
    zeros = (0,) * x.ndim
    return pl.BlockSpec(x.shape, lambda k: zeros, memory_space=space)


def picked(rows, cols, wanted):
    row = lax.broadcasted_iota(jnp.int32, (rows, cols), 0)
    col = lax.broadcasted_iota(jnp.int32, (rows, cols), 1)
    return jnp.where(row == wanted(col), 1.0, 0.0).astype(F32)


def opening_kernel(
    p_ref, inn_ref, sv_ref, mask_ref, w_ref, kx_ref, ky_ref, mw_ref, m_ref,
    split_ref, matrix_ref, innov_ref, static_ref, weight_ref, grad_ref, send_ref, cx_ref, cy_ref, scale_ref,
    s_ref, *, size,
):
    own = inn_ref.shape[1]
    shift = size.bit_length() - 1
    block, _, levels, _ = p_ref.shape
    members = mw_ref.shape[1]
    start = pl.program_id(0) * block

    @pl.when(pl.program_id(0) == 0)
    def _():
        for q in range(own):
            for v in range(VARS):
                for c in range(CB):
                    row = (q * VARS + v) * CB + c
                    lanes = slice(c * LANES, (c + 1) * LANES)
                    innov_ref[row : row + 1, :] = inn_ref[v, q : q + 1, lanes]
                    static_ref[row : row + 1, :] = sv_ref[v, q : q + 1, lanes]
                rows = slice((q * VARS + v) * CB, (q * VARS + v + 1) * CB)
                weight_ref[rows, :] = mask_ref[...].astype(F32) * w_ref[q, v]
        grad = weight_ref[...] * (0.0 - innov_ref[...])
        grad_ref[...] = grad
        rows = grad.shape[0]
        for d in range(size):
            send_ref[d * rows : (d + 1) * rows, :] = grad
        exact = lax.Precision.HIGHEST
        lane_bits = LANES.bit_length() - 1
        level = picked(levels, own * LANES, lambda c: own * (c & (size - 1)) + (c >> lane_bits))
        member = picked(members, members * size, lambda c: c >> shift)
        cx_ref[...] = jnp.dot(kx_ref[...], level, precision=exact, preferred_element_type=F32)
        cy_ref[...] = jnp.dot(ky_ref[...], level, precision=exact, preferred_element_type=F32)
        scale = jnp.dot(mw_ref[...], member, precision=exact, preferred_element_type=F32)
        scale_ref[...] = scale / float(size * members)
        matrix_ref[...] = m_ref[...]

    def one(k, carry):
        for v in range(VARS):
            for c in range(CB):
                s_ref[v * CB + c] = p_ref[k, v, :, c * LANES : (c + 1) * LANES].astype(F32)
        for v in range(VARS):
            for c in range(CB):
                for q in range(own):
                    split_ref[start + k, v, q, c] = s_ref[v * CB + c, pl.ds(q, size, stride=own), :]
        return carry

    lax.fori_loop(0, block, one, 0)


def opening(perturbations, innovation, static_var, obs_mask, obs_weight, kernel_x, kernel_y, member_weight, size):
    members, _, levels, _ = perturbations.shape
    own = levels // size
    block = math.gcd(members, 4)
    rows = own * ROWS
    small = [
        innovation, static_var, obs_mask.reshape(CB, LANES), obs_weight.T,
        kernel_x.T, kernel_y.T, member_weight.reshape(1, -1), jnp.asarray(interp_matrix(), BF16),
    ]
    specs = [whole(x, pltpu.SMEM if n == 3 else pltpu.VMEM) for n, x in enumerate(small)]
    shapes = (
        [jax.ShapeDtypeStruct((members, VARS, own, CB, size, LANES), F32), jax.ShapeDtypeStruct((CELLS, COLS), BF16)]
        + [jax.ShapeDtypeStruct((rows, LANES), F32)] * 4
        + [jax.ShapeDtypeStruct((size * rows, LANES), F32)]
        + [jax.ShapeDtypeStruct((5, own * LANES), F32)] * 2
        + [jax.ShapeDtypeStruct((1, members * size), F32)]
    )
    return pl.pallas_call(
        functools.partial(opening_kernel, size=size),
        grid=(members // block,),
        in_specs=[pl.BlockSpec((block, VARS, levels, COLS), lambda k: (k, 0, 0, 0))] + specs,
        out_specs=[vmem()] * len(shapes),
        out_shape=shapes,
        scratch_shapes=[pltpu.VMEM((VARS * CB, levels, LANES), F32)],
        compiler_params=grant(6),
        name="opening",
    )(*[in_hbm(x) for x in [perturbations] + small])


def project_kernel(p_ref, g_ref, m_ref, c_ref, near_ref, far_ref, hi_ref, lo_ref, *, chunks):
    odd = lax.axis_index("tile") % GRID_Y % 2
    edge = CELLS - 2 * CX
    near_at = pl.ds(pl.multiple_of((1 - odd) * edge, 8), 2 * CX)
    far_at = pl.ds(pl.multiple_of(odd * edge, 8), 2 * CX)
    members, _, _, _, owners, _ = p_ref.shape
    tiles = members * owners // LANES
    for n, q in enumerate(chunks):
        for c in range(CB):
            lanes = slice(c * LANES, (c + 1) * LANES)
            grad = [
                g_ref[pl.ds((n * VARS + v) * CB + c, owners, stride=len(chunks) * ROWS), :]
                for v in range(VARS)
            ]

            def one(k, carry):
                acc = p_ref[k, 0, q, c] * grad[0]
                for v in range(1, VARS):
                    acc = acc + p_ref[k, v, q, c] * grad[v]
                high, low = split_terms(acc)
                at = pl.ds(k * owners, owners)
                hi_ref[n, at, lanes] = high
                lo_ref[n, at, lanes] = low
                return carry

            lax.fori_loop(0, members, one, 0, unroll=True)
        dims = (((1,), (1,)), ((), ()))
        coarse = lax.dot_general(m_ref[...], hi_ref[n], dims, preferred_element_type=F32)
        coarse = coarse + lax.dot_general(m_ref[...], lo_ref[n], dims, preferred_element_type=F32)
        for t in range(tiles):
            piece = coarse[:, t * LANES : (t + 1) * LANES]
            c_ref[n * tiles + t] = piece
        for t in range(n * tiles, (n + 1) * tiles):
            near_ref[t] = c_ref[t, near_at, :]
            far_ref[t] = c_ref[t, far_at, :]


def project(split, gathered, matrix, chunks):
    members, _, _, _, owners, _ = split.shape
    tiles = len(chunks) * members * owners // LANES
    return pl.pallas_call(
        functools.partial(project_kernel, chunks=chunks),
        in_specs=[vmem(), vmem(), vmem()],
        out_specs=[vmem(), vmem(), vmem()],
        out_shape=[
            jax.ShapeDtypeStruct((tiles, CELLS, LANES), F32),
            jax.ShapeDtypeStruct((tiles, 2 * CX, LANES), F32),
            jax.ShapeDtypeStruct((tiles, 2 * CX, LANES), F32),
        ],
        scratch_shapes=[
            pltpu.VMEM((len(chunks), members * owners, COLS), BF16),
            pltpu.VMEM((len(chunks), members * owners, COLS), BF16),
        ],
        compiler_params=grant(8),
        name="project",
    )(split, gathered, matrix)


def sides(near, far, odd):
    return jnp.where(odd, near, far), jnp.where(odd, far, near)


def smooth_y_kernel(c_ref, near_ref, far_ref, k_ref, s_ref, xnear_ref, xfar_ref, *, chunks):
    tile = lax.axis_index("tile")
    odd_y, odd_x = tile % GRID_Y % 2 == 1, tile // GRID_Y % 2 == 1
    tiles = c_ref.shape[0]
    for t in range(tiles):
        q = chunks[t * len(chunks) // tiles]
        coef = [k_ref[d : d + 1, q * LANES : (q + 1) * LANES] for d in range(5)]
        before, after = sides(near_ref[t], far_ref[t], odd_y)

        def rows(b):
            if b < 0:
                return before[(b + 2) * CX : (b + 3) * CX, :]
            if b >= CY:
                return after[(b - CY) * CX : (b - CY + 1) * CX, :]
            return c_ref[t, b * CX : (b + 1) * CX, :]

        for b in range(CY):
            acc = coef[0] * rows(b - 2)
            for d in range(1, 5):
                acc = acc + coef[d] * rows(b + d - 2)
            s_ref[t, b * CX : (b + 1) * CX, :] = acc
        for j in range(2):
            low = s_ref[t, pl.ds(j, CY, stride=CX), :]
            high = s_ref[t, pl.ds(CX - 2 + j, CY, stride=CX), :]
            xnear_ref[t, j * CY : (j + 1) * CY, :], xfar_ref[t, j * CY : (j + 1) * CY, :] = sides(low, high, odd_x)


def smooth_y(coarse, near, far, coefs, chunks):
    tiles = coarse.shape[0]
    return pl.pallas_call(
        functools.partial(smooth_y_kernel, chunks=chunks),
        in_specs=[vmem()] * 4,
        out_specs=[vmem()] * 3,
        out_shape=[
            jax.ShapeDtypeStruct((tiles, CELLS, LANES), F32),
            jax.ShapeDtypeStruct((tiles, 2 * CY, LANES), F32),
            jax.ShapeDtypeStruct((tiles, 2 * CY, LANES), F32),
        ],
        compiler_params=grant(2),
        name="smooth_y",
    )(coarse, near, far, coefs)


def increment_kernel(p_ref, s_ref, near_ref, far_ref, k_ref, w_ref, m_ref, o_ref, e_ref, hi_ref, lo_ref, f_ref, *, chunks):
    odd_x = lax.axis_index("tile") // GRID_Y % 2 == 1
    members, _, _, _, owners, _ = p_ref.shape
    tiles = members * owners // LANES
    for n, q in enumerate(chunks):
        for t in range(tiles):
            at = n * tiles + t
            for b in range(CY):
                e_ref[at, b * EXT + 8 : b * EXT + 8 + CX, :] = s_ref[at, b * CX : (b + 1) * CX, :]
            before, after = sides(near_ref[at], far_ref[at], odd_x)
            for j in range(2):
                e_ref[at, pl.ds(6 + j, CY, stride=EXT), :] = before[j * CY : (j + 1) * CY, :]
                e_ref[at, pl.ds(8 + CX + j, CY, stride=EXT), :] = after[j * CY : (j + 1) * CY, :]
            scale = w_ref[:, t * LANES : (t + 1) * LANES]
            coef = [k_ref[d : d + 1, q * LANES : (q + 1) * LANES] * scale for d in range(5)]
            for b in range(CY):
                acc = coef[0] * e_ref[at, b * EXT + 6 : b * EXT + 6 + CX, :]
                for d in range(1, 5):
                    acc = acc + coef[d] * e_ref[at, b * EXT + 6 + d : b * EXT + 6 + d + CX, :]
                high, low = split_terms(acc)
                hi_ref[n, b * CX : (b + 1) * CX, t * LANES : (t + 1) * LANES] = high
                lo_ref[n, b * CX : (b + 1) * CX, t * LANES : (t + 1) * LANES] = low
        dims = (((0,), (0,)), ((), ()))
        fine = lax.dot_general(hi_ref[n], m_ref[...], dims, preferred_element_type=F32)
        f_ref[n] = fine + lax.dot_general(lo_ref[n], m_ref[...], dims, preferred_element_type=F32)
        for c in range(CB):
            lanes = slice(c * LANES, (c + 1) * LANES)

            def one(k, acc):
                at = pl.ds(k * owners, owners)
                local = f_ref[n, at, lanes]
                return tuple(acc[v] + p_ref[k, v, q, c] * local for v in range(VARS))

            zero = jnp.zeros((owners, LANES), F32)
            acc = lax.fori_loop(0, members, one, (zero,) * VARS, unroll=True)
            for v in range(VARS):
                o_ref[pl.ds((n * VARS + v) * CB + c, owners, stride=len(chunks) * ROWS), :] = acc[v]


def increment(split, smoothed, near, far, coefs, scale, matrix, chunks):
    members, _, _, _, owners, _ = split.shape
    return pl.pallas_call(
        functools.partial(increment_kernel, chunks=chunks),
        in_specs=[vmem()] * 7,
        out_specs=vmem(),
        out_shape=jax.ShapeDtypeStruct((owners * len(chunks) * ROWS, LANES), F32),
        scratch_shapes=[
            pltpu.VMEM((smoothed.shape[0], CY * EXT + 8, LANES), F32),
            pltpu.VMEM((len(chunks), CELLS, members * owners), BF16),
            pltpu.VMEM((len(chunks), CELLS, members * owners), BF16),
            pltpu.VMEM((len(chunks), members * owners, COLS), F32),
        ],
        compiler_params=grant(8),
        name="increment",
    )(split, smoothed, near, far, coefs, scale, matrix)


def update_kernel(r_ref, *refs, size, last):
    ins, outs = (refs[:3], refs[3:]) if last else (refs[:4], refs[4:])
    rows = ins[0].shape[0]
    total = r_ref[:rows, :]
    for d in range(1, size):
        total = total + r_ref[d * rows : (d + 1) * rows, :]
    if last:
        a_ref, g_ref, sv_ref = ins
        analysis = a_ref[...]
    else:
        g_ref, sv_ref, w_ref, inn_ref = ins
        analysis = jnp.zeros_like(total)
    inc = total + sv_ref[...] * g_ref[...]
    analysis = analysis - 0.5 * (analysis + inc)
    if last:
        own = rows // ROWS
        for q in range(own):
            for v in range(VARS):
                for c in range(CB):
                    row = (q * VARS + v) * CB + c
                    outs[0][v, q : q + 1, c * LANES : (c + 1) * LANES] = analysis[row : row + 1, :]
        return
    grad = w_ref[...] * (analysis - inn_ref[...])
    outs[0][...] = analysis
    outs[1][...] = grad
    for d in range(size):
        outs[2][d * rows : (d + 1) * rows, :] = grad


def update(received, args, size, last):
    rows = received.shape[0] // size
    flat = jax.ShapeDtypeStruct((rows, LANES), F32)
    if last:
        shapes = [jax.ShapeDtypeStruct((VARS, rows // ROWS, COLS), F32)]
    else:
        shapes = [flat, flat, jax.ShapeDtypeStruct((size * rows, LANES), F32)]
    return pl.pallas_call(
        functools.partial(update_kernel, size=size, last=last),
        in_specs=[vmem()] * (1 + len(args)),
        out_specs=[vmem()] * len(shapes),
        out_shape=shapes,
        compiler_params=grant(2),
        name="update",
    )(received, *args)


def exchange(x, size):
    blocks = x.reshape(size, -1, LANES)
    return lax.all_to_all(blocks, "mem", 0, 0, tiled=True).reshape(x.shape)


def swapped(near, far, stride, places, periodic):
    def pairs(is_near):
        out = []
        for i in range(lax.axis_size("tile")):
            place = i // stride % places
            to = place + (1 if (place % 2 == 0) == is_near else -1)
            if periodic or 0 <= to < places:
                out.append((i, i + (to % places - place) * stride))
        return out

    from_far = lax.ppermute(far, "tile", pairs(False))
    from_near = lax.ppermute(near, "tile", pairs(True))
    return from_near, from_far


def body(perturbations, member_weight, innovation, obs_weight, static_var, obs_mask, kernel_x, kernel_y):
    size = lax.axis_size("mem")
    grid_x = lax.axis_size("tile") // GRID_Y
    chunks = tuple(range(perturbations.shape[2] // size))
    split, matrix, innov, static, weight, gradient, to_send, coef_x, coef_y, scale = opening(
        perturbations, innovation, static_var, obs_mask, obs_weight, kernel_x, kernel_y, member_weight, size
    )
    analysis = None
    for step in range(STEPS):
        gathered = exchange(to_send, size)
        coarse, near, far = project(split, gathered, matrix, chunks)
        near, far = swapped(near, far, 1, GRID_Y, False)
        smoothed, near, far = smooth_y(coarse, near, far, coef_y, chunks)
        near, far = swapped(near, far, GRID_Y, grid_x, True)
        partial = increment(split, smoothed, near, far, coef_x, scale, matrix, chunks)
        received = exchange(partial, size)
        if step == STEPS - 1:
            return update(received, (analysis, gradient, static), size, True)[0]
        analysis, gradient, to_send = update(received, (gradient, static, weight, innov), size, False)


def solution(mesh):
    placed = (
        P("mem", None, None, "tile"),
        P("mem"),
        P(None, "mem", "tile"),
        P(None, "mem"),
        P(None, "mem", "tile"),
        P("tile"),
        P(),
        P(),
    )
    return jax.shard_map(
        body, mesh=mesh, in_specs=placed, out_specs=P(None, "mem", "tile"), check_vma=False
    )
```

```python
import functools
import math

import jax
import jax.numpy as jnp
import numpy as np
from jax import lax
from jax.experimental import pallas as pl
from jax.experimental.pallas import tpu as pltpu
from jax.sharding import PartitionSpec as P


VARS = 3
TILE_X = 32
TILE_Y = 32
GRID_Y = 4
STEPS = 2
CX = TILE_X // 2
CY = TILE_Y // 2
CELLS = CX * CY
COLS = TILE_X * TILE_Y
LANES = 128
CB = COLS // LANES
ROWS = VARS * CB
EXT = CX + 8
F32 = jnp.float32
BF16 = jnp.bfloat16


def interp_rows(fine_count):
    coarse_count = fine_count // 2
    rows = np.zeros((fine_count, coarse_count), np.float32)
    for i in range(fine_count):
        upper = 0.75 if i % 2 == 0 else 0.25
        low = (i - 1) // 2
        rows[i, min(max(low, 0), coarse_count - 1)] += 1.0 - upper
        rows[i, min(max(low + 1, 0), coarse_count - 1)] += upper
    return rows


def interp_matrix():
    rows_x, rows_y = interp_rows(TILE_X), interp_rows(TILE_Y)
    full = np.einsum("ia,jb->baij", rows_x, rows_y)
    return full.reshape(CELLS, COLS)


def edge_matrix():
    rows = interp_matrix().reshape(CY, CX, COLS)[:, [0, 1, CX - 2, CX - 1]]
    rows = rows.transpose(1, 0, 2).reshape(4 * CY, CB, LANES)
    blocks = [c for c in range(CB) if rows[:, c].any()]
    return rows[:, blocks].reshape(4 * CY, -1), blocks


def vmem():
    return pl.BlockSpec(memory_space=pltpu.VMEM)


def grant(mib):
    return pltpu.CompilerParams(vmem_limit_bytes=mib * 1024 * 1024)


def split_terms(x):
    high = x.astype(BF16)
    return high, (x - high.astype(F32)).astype(BF16)


def in_hbm(x):
    return pltpu.with_memory_space_constraint(x, pltpu.HBM)


def whole(x, space=pltpu.VMEM):
    zeros = (0,) * x.ndim
    return pl.BlockSpec(x.shape, lambda k: zeros, memory_space=space)


def picked(rows, cols, wanted):
    row = lax.broadcasted_iota(jnp.int32, (rows, cols), 0)
    col = lax.broadcasted_iota(jnp.int32, (rows, cols), 1)
    return jnp.where(row == wanted(col), 1.0, 0.0).astype(F32)


def opening_kernel(
    p_ref, inn_ref, sv_ref, mask_ref, w_ref, kx_ref, ky_ref, mw_ref, m_ref, ed_ref,
    split_ref, matrix_ref, edge_ref, innov_ref, static_ref, weight_ref, grad_ref, send_ref, cx_ref, cy_ref, scale_ref,
    s_ref, *, size,
):
    own = inn_ref.shape[1]
    shift = size.bit_length() - 1
    block, _, levels, _ = p_ref.shape
    members = mw_ref.shape[1]
    start = pl.program_id(0) * block

    @pl.when(pl.program_id(0) == 0)
    def _():
        for q in range(own):
            for v in range(VARS):
                for c in range(CB):
                    row = (q * VARS + v) * CB + c
                    lanes = slice(c * LANES, (c + 1) * LANES)
                    innov_ref[row : row + 1, :] = inn_ref[v, q : q + 1, lanes]
                    static_ref[row : row + 1, :] = sv_ref[v, q : q + 1, lanes]
                rows = slice((q * VARS + v) * CB, (q * VARS + v + 1) * CB)
                weight_ref[rows, :] = mask_ref[...].astype(F32) * w_ref[q, v]
        grad = weight_ref[...] * (0.0 - innov_ref[...])
        grad_ref[...] = grad
        rows = grad.shape[0]
        for d in range(size):
            send_ref[d * rows : (d + 1) * rows, :] = grad
        exact = lax.Precision.HIGHEST
        lane_bits = LANES.bit_length() - 1
        level = picked(levels, own * LANES, lambda c: own * (c & (size - 1)) + (c >> lane_bits))
        member = picked(members, members * size, lambda c: c >> shift)
        cx_ref[...] = jnp.dot(kx_ref[...], level, precision=exact, preferred_element_type=F32)
        cy_ref[...] = jnp.dot(ky_ref[...], level, precision=exact, preferred_element_type=F32)
        scale = jnp.dot(mw_ref[...], member, precision=exact, preferred_element_type=F32)
        scale_ref[...] = scale / float(size * members)
        matrix_ref[...] = m_ref[...]
        edge_ref[...] = ed_ref[...]

    def one(k, carry):
        for v in range(VARS):
            for c in range(CB):
                s_ref[v * CB + c] = p_ref[k, v, :, c * LANES : (c + 1) * LANES].astype(F32)
        for v in range(VARS):
            for c in range(CB):
                for q in range(own):
                    split_ref[start + k, v, q, c] = s_ref[v * CB + c, pl.ds(q, size, stride=own), :]
        return carry

    lax.fori_loop(0, block, one, 0)


def opening(perturbations, innovation, static_var, obs_mask, obs_weight, kernel_x, kernel_y, member_weight, size):
    members, _, levels, _ = perturbations.shape
    own = levels // size
    block = math.gcd(members, 4)
    rows = own * ROWS
    small = [
        innovation, static_var, obs_mask.reshape(CB, LANES), obs_weight.T,
        kernel_x.T, kernel_y.T, member_weight.reshape(1, -1), jnp.asarray(interp_matrix(), BF16),
        jnp.asarray(edge_matrix()[0], BF16),
    ]
    specs = [whole(x, pltpu.SMEM if n == 3 else pltpu.VMEM) for n, x in enumerate(small)]
    shapes = (
        [jax.ShapeDtypeStruct((members, VARS, own, CB, size, LANES), F32), jax.ShapeDtypeStruct((CELLS, COLS), BF16)]
        + [jax.ShapeDtypeStruct(small[-1].shape, BF16)]
        + [jax.ShapeDtypeStruct((rows, LANES), F32)] * 4
        + [jax.ShapeDtypeStruct((size * rows, LANES), F32)]
        + [jax.ShapeDtypeStruct((5, own * LANES), F32)] * 2
        + [jax.ShapeDtypeStruct((1, members * size), F32)]
    )
    return pl.pallas_call(
        functools.partial(opening_kernel, size=size),
        grid=(members // block,),
        in_specs=[pl.BlockSpec((block, VARS, levels, COLS), lambda k: (k, 0, 0, 0))] + specs,
        out_specs=[vmem()] * len(shapes),
        out_shape=shapes,
        scratch_shapes=[pltpu.VMEM((VARS * CB, levels, LANES), F32)],
        compiler_params=grant(6),
        name="opening",
    )(*[in_hbm(x) for x in [perturbations] + small])


def project_kernel(p_ref, g_ref, m_ref, c_ref, near_ref, far_ref, hi_ref, lo_ref, *, chunks):
    odd = lax.axis_index("tile") % GRID_Y % 2
    edge = CELLS - 2 * CX
    near_at = pl.ds(pl.multiple_of((1 - odd) * edge, 8), 2 * CX)
    far_at = pl.ds(pl.multiple_of(odd * edge, 8), 2 * CX)
    members, _, _, _, owners, _ = p_ref.shape
    tiles = members * owners // LANES
    for n, q in enumerate(chunks):
        for c in range(CB):
            lanes = slice(c * LANES, (c + 1) * LANES)
            grad = [
                g_ref[pl.ds((n * VARS + v) * CB + c, owners, stride=len(chunks) * ROWS), :]
                for v in range(VARS)
            ]

            def one(k, carry):
                acc = p_ref[k, 0, q, c] * grad[0]
                for v in range(1, VARS):
                    acc = acc + p_ref[k, v, q, c] * grad[v]
                high, low = split_terms(acc)
                at = pl.ds(k * owners, owners)
                hi_ref[n, at, lanes] = high
                lo_ref[n, at, lanes] = low
                return carry

            lax.fori_loop(0, members, one, 0, unroll=True)
        dims = (((1,), (1,)), ((), ()))
        coarse = lax.dot_general(m_ref[...], hi_ref[n], dims, preferred_element_type=F32)
        coarse = coarse + lax.dot_general(m_ref[...], lo_ref[n], dims, preferred_element_type=F32)
        for t in range(tiles):
            piece = coarse[:, t * LANES : (t + 1) * LANES]
            c_ref[n * tiles + t] = piece
        for t in range(n * tiles, (n + 1) * tiles):
            near_ref[t] = c_ref[t, near_at, :]
            far_ref[t] = c_ref[t, far_at, :]


def project(split, gathered, matrix, chunks):
    members, _, _, _, owners, _ = split.shape
    tiles = len(chunks) * members * owners // LANES
    return pl.pallas_call(
        functools.partial(project_kernel, chunks=chunks),
        in_specs=[vmem(), vmem(), vmem()],
        out_specs=[vmem(), vmem(), vmem()],
        out_shape=[
            jax.ShapeDtypeStruct((tiles, CELLS, LANES), F32),
            jax.ShapeDtypeStruct((tiles, 2 * CX, LANES), F32),
            jax.ShapeDtypeStruct((tiles, 2 * CX, LANES), F32),
        ],
        scratch_shapes=[
            pltpu.VMEM((len(chunks), members * owners, COLS), BF16),
            pltpu.VMEM((len(chunks), members * owners, COLS), BF16),
        ],
        compiler_params=grant(8),
        name="project",
    )(split, gathered, matrix)


def sides(near, far, odd):
    return jnp.where(odd, near, far), jnp.where(odd, far, near)


def smooth_y_kernel(c_ref, near_ref, far_ref, k_ref, s_ref, xnear_ref, xfar_ref, *, chunks):
    tile = lax.axis_index("tile")
    odd_y, odd_x = tile % GRID_Y % 2 == 1, tile // GRID_Y % 2 == 1
    tiles = c_ref.shape[0]
    for t in range(tiles):
        q = chunks[t * len(chunks) // tiles]
        coef = [k_ref[d : d + 1, q * LANES : (q + 1) * LANES] for d in range(5)]
        before, after = sides(near_ref[t], far_ref[t], odd_y)

        def rows(b):
            if b < 0:
                return before[(b + 2) * CX : (b + 3) * CX, :]
            if b >= CY:
                return after[(b - CY) * CX : (b - CY + 1) * CX, :]
            return c_ref[t, b * CX : (b + 1) * CX, :]

        for b in range(CY):
            acc = coef[0] * rows(b - 2)
            for d in range(1, 5):
                acc = acc + coef[d] * rows(b + d - 2)
            s_ref[t, b * CX : (b + 1) * CX, :] = acc
        for j in range(2):
            low = s_ref[t, pl.ds(j, CY, stride=CX), :]
            high = s_ref[t, pl.ds(CX - 2 + j, CY, stride=CX), :]
            xnear_ref[t, j * CY : (j + 1) * CY, :], xfar_ref[t, j * CY : (j + 1) * CY, :] = sides(low, high, odd_x)


def smooth_y(coarse, near, far, coefs, chunks):
    tiles = coarse.shape[0]
    return pl.pallas_call(
        functools.partial(smooth_y_kernel, chunks=chunks),
        in_specs=[vmem()] * 4,
        out_specs=[vmem()] * 3,
        out_shape=[
            jax.ShapeDtypeStruct((tiles, CELLS, LANES), F32),
            jax.ShapeDtypeStruct((tiles, 2 * CY, LANES), F32),
            jax.ShapeDtypeStruct((tiles, 2 * CY, LANES), F32),
        ],
        compiler_params=grant(2),
        name="smooth_y",
    )(coarse, near, far, coefs)


def interior_kernel(p_ref, s_ref, k_ref, w_ref, m_ref, o_ref, e_ref, hi_ref, lo_ref, f_ref, *, chunks):
    members, _, _, _, owners, _ = p_ref.shape
    tiles = members * owners // LANES
    for n, q in enumerate(chunks):
        for t in range(tiles):
            at = n * tiles + t
            for b in range(CY):
                e_ref[at, b * EXT + 8 : b * EXT + 8 + CX, :] = s_ref[at, b * CX : (b + 1) * CX, :]
            for j in (6, 7, 8 + CX, 9 + CX):
                e_ref[at, pl.ds(j, CY, stride=EXT), :] = jnp.zeros((CY, LANES), F32)
            scale = w_ref[:, t * LANES : (t + 1) * LANES]
            coef = [k_ref[d : d + 1, q * LANES : (q + 1) * LANES] * scale for d in range(5)]
            for b in range(CY):
                acc = coef[0] * e_ref[at, b * EXT + 6 : b * EXT + 6 + CX, :]
                for d in range(1, 5):
                    acc = acc + coef[d] * e_ref[at, b * EXT + 6 + d : b * EXT + 6 + d + CX, :]
                high, low = split_terms(acc)
                hi_ref[n, b * CX : (b + 1) * CX, t * LANES : (t + 1) * LANES] = high
                lo_ref[n, b * CX : (b + 1) * CX, t * LANES : (t + 1) * LANES] = low
        dims = (((0,), (0,)), ((), ()))
        fine = lax.dot_general(hi_ref[n], m_ref[...], dims, preferred_element_type=F32)
        f_ref[n] = fine + lax.dot_general(lo_ref[n], m_ref[...], dims, preferred_element_type=F32)
        for c in range(CB):
            lanes = slice(c * LANES, (c + 1) * LANES)

            def one(k, acc):
                at = pl.ds(k * owners, owners)
                local = f_ref[n, at, lanes]
                return tuple(acc[v] + p_ref[k, v, q, c] * local for v in range(VARS))

            zero = jnp.zeros((owners, LANES), F32)
            acc = lax.fori_loop(0, members, one, (zero,) * VARS, unroll=True)
            for v in range(VARS):
                o_ref[pl.ds((n * VARS + v) * CB + c, owners, stride=len(chunks) * ROWS), :] = acc[v]


def interior(split, smoothed, coefs, scale, matrix, chunks):
    members, _, _, _, owners, _ = split.shape
    return pl.pallas_call(
        functools.partial(interior_kernel, chunks=chunks),
        in_specs=[vmem()] * 5,
        out_specs=vmem(),
        out_shape=jax.ShapeDtypeStruct((owners * len(chunks) * ROWS, LANES), F32),
        scratch_shapes=[
            pltpu.VMEM((smoothed.shape[0], CY * EXT + 8, LANES), F32),
            pltpu.VMEM((len(chunks), CELLS, members * owners), BF16),
            pltpu.VMEM((len(chunks), CELLS, members * owners), BF16),
            pltpu.VMEM((len(chunks), members * owners, COLS), F32),
        ],
        compiler_params=grant(8),
        name="interior",
    )(split, smoothed, coefs, scale, matrix)


def halo_kernel(p_ref, l_ref, near_ref, far_ref, k_ref, w_ref, m_ref, o_ref, hi_ref, lo_ref, f_ref, *, chunks, blocks):
    odd_x = lax.axis_index("tile") // GRID_Y % 2 == 1
    members, _, _, _, owners, _ = p_ref.shape
    tiles = members * owners // LANES
    stride = len(chunks) * ROWS
    o_ref[...] = l_ref[...]
    for n, q in enumerate(chunks):
        for t in range(tiles):
            before, after = sides(near_ref[n * tiles + t], far_ref[n * tiles + t], odd_x)
            scale = w_ref[:, t * LANES : (t + 1) * LANES]
            coef = [k_ref[d : d + 1, q * LANES : (q + 1) * LANES] * scale for d in range(5)]
            cells = [
                coef[0] * before[:CY] + coef[1] * before[CY:],
                coef[0] * before[CY:],
                coef[4] * after[:CY],
                coef[3] * after[:CY] + coef[4] * after[CY:],
            ]
            for e, cell in enumerate(cells):
                high, low = split_terms(cell)
                hi_ref[n, e * CY : (e + 1) * CY, t * LANES : (t + 1) * LANES] = high
                lo_ref[n, e * CY : (e + 1) * CY, t * LANES : (t + 1) * LANES] = low
        dims = (((0,), (0,)), ((), ()))
        fine = lax.dot_general(hi_ref[n], m_ref[...], dims, preferred_element_type=F32)
        f_ref[n] = fine + lax.dot_general(lo_ref[n], m_ref[...], dims, preferred_element_type=F32)
        for i, c in enumerate(blocks):
            acc = [jnp.zeros((owners, LANES), F32)] * VARS
            for k in range(members):
                local = f_ref[n, k * owners : (k + 1) * owners, i * LANES : (i + 1) * LANES]
                acc = [acc[v] + p_ref[k, v, q, c] * local for v in range(VARS)]
            for v in range(VARS):
                at = pl.ds((n * VARS + v) * CB + c, owners, stride=stride)
                o_ref[at, :] = l_ref[at, :] + acc[v]


def halo_part(split, partial, near, far, coefs, scale, edge, chunks):
    members, _, _, _, owners, _ = split.shape
    return pl.pallas_call(
        functools.partial(halo_kernel, chunks=chunks, blocks=edge_matrix()[1]),
        in_specs=[vmem()] * 7,
        out_specs=vmem(),
        out_shape=jax.ShapeDtypeStruct(partial.shape, F32),
        scratch_shapes=[
            pltpu.VMEM((len(chunks), edge.shape[0], members * owners), BF16),
            pltpu.VMEM((len(chunks), edge.shape[0], members * owners), BF16),
            pltpu.VMEM((len(chunks), members * owners, edge.shape[1]), F32),
        ],
        compiler_params=grant(6),
        name="halo_part",
    )(split, partial, near, far, coefs, scale, edge)


def update_kernel(r_ref, *refs, size, last):
    ins, outs = (refs[:3], refs[3:]) if last else (refs[:4], refs[4:])
    rows = ins[0].shape[0]
    total = r_ref[:rows, :]
    for d in range(1, size):
        total = total + r_ref[d * rows : (d + 1) * rows, :]
    if last:
        a_ref, g_ref, sv_ref = ins
        analysis = a_ref[...]
    else:
        g_ref, sv_ref, w_ref, inn_ref = ins
        analysis = jnp.zeros_like(total)
    inc = total + sv_ref[...] * g_ref[...]
    analysis = analysis - 0.5 * (analysis + inc)
    if last:
        own = rows // ROWS
        for q in range(own):
            for v in range(VARS):
                for c in range(CB):
                    row = (q * VARS + v) * CB + c
                    outs[0][v, q : q + 1, c * LANES : (c + 1) * LANES] = analysis[row : row + 1, :]
        return
    grad = w_ref[...] * (analysis - inn_ref[...])
    outs[0][...] = analysis
    outs[1][...] = grad
    for d in range(size):
        outs[2][d * rows : (d + 1) * rows, :] = grad


def update(received, args, size, last):
    rows = received.shape[0] // size
    flat = jax.ShapeDtypeStruct((rows, LANES), F32)
    if last:
        shapes = [jax.ShapeDtypeStruct((VARS, rows // ROWS, COLS), F32)]
    else:
        shapes = [flat, flat, jax.ShapeDtypeStruct((size * rows, LANES), F32)]
    return pl.pallas_call(
        functools.partial(update_kernel, size=size, last=last),
        in_specs=[vmem()] * (1 + len(args)),
        out_specs=[vmem()] * len(shapes),
        out_shape=shapes,
        compiler_params=grant(2),
        name="update",
    )(received, *args)


def exchange(x, size):
    blocks = x.reshape(size, -1, LANES)
    return lax.all_to_all(blocks, "mem", 0, 0, tiled=True).reshape(x.shape)


def swapped(near, far, stride, places, periodic):
    def pairs(is_near):
        out = []
        for i in range(lax.axis_size("tile")):
            place = i // stride % places
            to = place + (1 if (place % 2 == 0) == is_near else -1)
            if periodic or 0 <= to < places:
                out.append((i, i + (to % places - place) * stride))
        return out

    from_far = lax.ppermute(far, "tile", pairs(False))
    from_near = lax.ppermute(near, "tile", pairs(True))
    return from_near, from_far


def body(perturbations, member_weight, innovation, obs_weight, static_var, obs_mask, kernel_x, kernel_y):
    size = lax.axis_size("mem")
    grid_x = lax.axis_size("tile") // GRID_Y
    chunks = tuple(range(perturbations.shape[2] // size))
    split, matrix, edge, innov, static, weight, gradient, to_send, coef_x, coef_y, scale = opening(
        perturbations, innovation, static_var, obs_mask, obs_weight, kernel_x, kernel_y, member_weight, size
    )
    analysis = None
    for step in range(STEPS):
        gathered = exchange(to_send, size)
        coarse, near, far = project(split, gathered, matrix, chunks)
        near, far = swapped(near, far, 1, GRID_Y, False)
        smoothed, near, far = smooth_y(coarse, near, far, coef_y, chunks)
        near, far = swapped(near, far, GRID_Y, grid_x, True)
        partial = interior(split, smoothed, coef_x, scale, matrix, chunks)
        partial = halo_part(split, partial, near, far, coef_x, scale, edge, chunks)
        received = exchange(partial, size)
        if step == STEPS - 1:
            return update(received, (analysis, gradient, static), size, True)[0]
        analysis, gradient, to_send = update(received, (gradient, static, weight, innov), size, False)


def solution(mesh):
    placed = (
        P("mem", None, None, "tile"),
        P("mem"),
        P(None, "mem", "tile"),
        P(None, "mem"),
        P(None, "mem", "tile"),
        P("tile"),
        P(),
        P(),
    )
    return jax.shard_map(
        body, mesh=mesh, in_specs=placed, out_specs=P(None, "mem", "tile"), check_vma=False
    )
```

```python
import functools
import math

import jax
import jax.numpy as jnp
import numpy as np
from jax import lax
from jax.experimental import pallas as pl
from jax.experimental.pallas import tpu as pltpu
from jax.sharding import PartitionSpec as P


VARS = 3
TILE_X = 32
TILE_Y = 32
GRID_Y = 4
STEPS = 2
CX = TILE_X // 2
CY = TILE_Y // 2
CELLS = CX * CY
COLS = TILE_X * TILE_Y
LANES = 128
CB = COLS // LANES
ROWS = VARS * CB
EXT = CX + 8
F32 = jnp.float32
BF16 = jnp.bfloat16


def interp_rows(fine_count):
    coarse_count = fine_count // 2
    rows = np.zeros((fine_count, coarse_count), np.float32)
    for i in range(fine_count):
        upper = 0.75 if i % 2 == 0 else 0.25
        low = (i - 1) // 2
        rows[i, min(max(low, 0), coarse_count - 1)] += 1.0 - upper
        rows[i, min(max(low + 1, 0), coarse_count - 1)] += upper
    return rows


def interp_matrix():
    rows_x, rows_y = interp_rows(TILE_X), interp_rows(TILE_Y)
    full = np.einsum("ia,jb->baij", rows_x, rows_y)
    return full.reshape(CELLS, COLS)


def edge_matrix():
    rows = interp_matrix().reshape(CY, CX, COLS)[:, [0, 1, CX - 2, CX - 1]]
    rows = rows.transpose(1, 0, 2).reshape(4 * CY, CB, LANES)
    blocks = [c for c in range(CB) if rows[:, c].any()]
    return rows[:, blocks].reshape(4 * CY, -1), blocks


def vmem():
    return pl.BlockSpec(memory_space=pltpu.VMEM)


def grant(mib):
    return pltpu.CompilerParams(vmem_limit_bytes=mib * 1024 * 1024)


def split_terms(x):
    high = x.astype(BF16)
    return high, (x - high.astype(F32)).astype(BF16)


def in_hbm(x):
    return pltpu.with_memory_space_constraint(x, pltpu.HBM)


def whole(x, space=pltpu.VMEM):
    zeros = (0,) * x.ndim
    return pl.BlockSpec(x.shape, lambda k: zeros, memory_space=space)


def picked(rows, cols, wanted):
    row = lax.broadcasted_iota(jnp.int32, (rows, cols), 0)
    col = lax.broadcasted_iota(jnp.int32, (rows, cols), 1)
    return jnp.where(row == wanted(col), 1.0, 0.0).astype(F32)


def opening_kernel(
    p_ref, inn_ref, sv_ref, mask_ref, w_ref, kx_ref, ky_ref, mw_ref, m_ref, ed_ref,
    split_ref, matrix_ref, edge_ref, innov_ref, static_ref, weight_ref, grad_ref, send_ref, cx_ref, cy_ref, scale_ref,
    s_ref, *, size, steps,
):
    own = inn_ref.shape[1]
    shift = size.bit_length() - 1
    block, _, levels, _ = p_ref.shape
    members = mw_ref.shape[1]
    start = pl.program_id(0) * block

    def at_step(n):
        return pl.when(pl.program_id(0) == min(n, steps - 1))

    @at_step(0)
    def _():
        for q in range(own):
            for v in range(VARS):
                for c in range(CB):
                    row = (q * VARS + v) * CB + c
                    innov_ref[row : row + 1, :] = inn_ref[v, q : q + 1, c * LANES : (c + 1) * LANES]
                rows = slice((q * VARS + v) * CB, (q * VARS + v + 1) * CB)
                weight_ref[rows, :] = mask_ref[...].astype(F32) * w_ref[q, v]
        grad = weight_ref[...] * (0.0 - innov_ref[...])
        grad_ref[...] = grad
        rows = grad.shape[0]
        for d in range(size):
            send_ref[d * rows : (d + 1) * rows, :] = grad

    @at_step(1)
    def _():
        exact = lax.Precision.HIGHEST
        lane_bits = LANES.bit_length() - 1
        level = picked(levels, own * LANES, lambda c: own * (c & (size - 1)) + (c >> lane_bits))
        cx_ref[...] = jnp.dot(kx_ref[...], level, precision=exact, preferred_element_type=F32)
        cy_ref[...] = jnp.dot(ky_ref[...], level, precision=exact, preferred_element_type=F32)

    @at_step(2)
    def _():
        member = picked(members, members * size, lambda c: c >> shift)
        exact = lax.Precision.HIGHEST
        scale = jnp.dot(mw_ref[...], member, precision=exact, preferred_element_type=F32)
        scale_ref[...] = scale / float(size * members)

    @at_step(3)
    def _():
        matrix_ref[...] = m_ref[...]
        edge_ref[...] = ed_ref[...]

    @at_step(4)
    def _():
        for q in range(own):
            for v in range(VARS):
                for c in range(CB):
                    row = (q * VARS + v) * CB + c
                    static_ref[row : row + 1, :] = sv_ref[v, q : q + 1, c * LANES : (c + 1) * LANES]

    def one(k, carry):
        for v in range(VARS):
            for c in range(CB):
                s_ref[v * CB + c] = p_ref[k, v, :, c * LANES : (c + 1) * LANES].astype(F32)
        for v in range(VARS):
            for c in range(CB):
                for q in range(own):
                    split_ref[start + k, v, q, c] = s_ref[v * CB + c, pl.ds(q, size, stride=own), :]
        return carry

    lax.fori_loop(0, block, one, 0)


def opening(perturbations, innovation, static_var, obs_mask, obs_weight, kernel_x, kernel_y, member_weight, size):
    members, _, levels, _ = perturbations.shape
    own = levels // size
    block = math.gcd(members, 4)
    rows = own * ROWS
    small = [
        innovation, static_var, obs_mask.reshape(CB, LANES), obs_weight.T,
        kernel_x.T, kernel_y.T, member_weight.reshape(1, -1), jnp.asarray(interp_matrix(), BF16),
        jnp.asarray(edge_matrix()[0], BF16),
    ]
    specs = [whole(x, pltpu.SMEM if n == 3 else pltpu.VMEM) for n, x in enumerate(small)]
    shapes = (
        [jax.ShapeDtypeStruct((members, VARS, own, CB, size, LANES), F32), jax.ShapeDtypeStruct((CELLS, COLS), BF16)]
        + [jax.ShapeDtypeStruct(small[-1].shape, BF16)]
        + [jax.ShapeDtypeStruct((rows, LANES), F32)] * 4
        + [jax.ShapeDtypeStruct((size * rows, LANES), F32)]
        + [jax.ShapeDtypeStruct((5, own * LANES), F32)] * 2
        + [jax.ShapeDtypeStruct((1, members * size), F32)]
    )
    return pl.pallas_call(
        functools.partial(opening_kernel, size=size, steps=members // block),
        grid=(members // block,),
        in_specs=[pl.BlockSpec((block, VARS, levels, COLS), lambda k: (k, 0, 0, 0))] + specs,
        out_specs=[vmem()] * len(shapes),
        out_shape=shapes,
        scratch_shapes=[pltpu.VMEM((VARS * CB, levels, LANES), F32)],
        compiler_params=grant(6),
        name="opening",
    )(*[in_hbm(x) for x in [perturbations] + small])


def project_kernel(p_ref, g_ref, m_ref, c_ref, near_ref, far_ref, hi_ref, lo_ref, *, chunks):
    odd = lax.axis_index("tile") % GRID_Y % 2
    edge = CELLS - 2 * CX
    near_at = pl.ds(pl.multiple_of((1 - odd) * edge, 8), 2 * CX)
    far_at = pl.ds(pl.multiple_of(odd * edge, 8), 2 * CX)
    members, _, _, _, owners, _ = p_ref.shape
    tiles = members * owners // LANES
    for n, q in enumerate(chunks):
        for c in range(CB):
            lanes = slice(c * LANES, (c + 1) * LANES)
            grad = [
                g_ref[pl.ds((n * VARS + v) * CB + c, owners, stride=len(chunks) * ROWS), :]
                for v in range(VARS)
            ]

            def one(k, carry):
                acc = p_ref[k, 0, q, c] * grad[0]
                for v in range(1, VARS):
                    acc = acc + p_ref[k, v, q, c] * grad[v]
                high, low = split_terms(acc)
                at = pl.ds(k * owners, owners)
                hi_ref[n, at, lanes] = high
                lo_ref[n, at, lanes] = low
                return carry

            lax.fori_loop(0, members, one, 0, unroll=True)
        dims = (((1,), (1,)), ((), ()))
        coarse = lax.dot_general(m_ref[...], hi_ref[n], dims, preferred_element_type=F32)
        coarse = coarse + lax.dot_general(m_ref[...], lo_ref[n], dims, preferred_element_type=F32)
        for t in range(tiles):
            piece = coarse[:, t * LANES : (t + 1) * LANES]
            c_ref[n * tiles + t] = piece
        for t in range(n * tiles, (n + 1) * tiles):
            near_ref[t] = c_ref[t, near_at, :]
            far_ref[t] = c_ref[t, far_at, :]


def project(split, gathered, matrix, chunks):
    members, _, _, _, owners, _ = split.shape
    tiles = len(chunks) * members * owners // LANES
    return pl.pallas_call(
        functools.partial(project_kernel, chunks=chunks),
        in_specs=[vmem(), vmem(), vmem()],
        out_specs=[vmem(), vmem(), vmem()],
        out_shape=[
            jax.ShapeDtypeStruct((tiles, CELLS, LANES), F32),
            jax.ShapeDtypeStruct((tiles, 2 * CX, LANES), F32),
            jax.ShapeDtypeStruct((tiles, 2 * CX, LANES), F32),
        ],
        scratch_shapes=[
            pltpu.VMEM((len(chunks), members * owners, COLS), BF16),
            pltpu.VMEM((len(chunks), members * owners, COLS), BF16),
        ],
        compiler_params=grant(8),
        name="project",
    )(split, gathered, matrix)


def sides(near, far, odd):
    return jnp.where(odd, near, far), jnp.where(odd, far, near)


def smooth_y_kernel(c_ref, near_ref, far_ref, k_ref, s_ref, xnear_ref, xfar_ref, *, chunks):
    tile = lax.axis_index("tile")
    odd_y, odd_x = tile % GRID_Y % 2 == 1, tile // GRID_Y % 2 == 1
    tiles = c_ref.shape[0]
    for t in range(tiles):
        q = chunks[t * len(chunks) // tiles]
        coef = [k_ref[d : d + 1, q * LANES : (q + 1) * LANES] for d in range(5)]
        before, after = sides(near_ref[t], far_ref[t], odd_y)

        def rows(b):
            if b < 0:
                return before[(b + 2) * CX : (b + 3) * CX, :]
            if b >= CY:
                return after[(b - CY) * CX : (b - CY + 1) * CX, :]
            return c_ref[t, b * CX : (b + 1) * CX, :]

        for b in range(CY):
            acc = coef[0] * rows(b - 2)
            for d in range(1, 5):
                acc = acc + coef[d] * rows(b + d - 2)
            s_ref[t, b * CX : (b + 1) * CX, :] = acc
        for j in range(2):
            low = s_ref[t, pl.ds(j, CY, stride=CX), :]
            high = s_ref[t, pl.ds(CX - 2 + j, CY, stride=CX), :]
            xnear_ref[t, j * CY : (j + 1) * CY, :], xfar_ref[t, j * CY : (j + 1) * CY, :] = sides(low, high, odd_x)


def smooth_y(coarse, near, far, coefs, chunks):
    tiles = coarse.shape[0]
    return pl.pallas_call(
        functools.partial(smooth_y_kernel, chunks=chunks),
        in_specs=[vmem()] * 4,
        out_specs=[vmem()] * 3,
        out_shape=[
            jax.ShapeDtypeStruct((tiles, CELLS, LANES), F32),
            jax.ShapeDtypeStruct((tiles, 2 * CY, LANES), F32),
            jax.ShapeDtypeStruct((tiles, 2 * CY, LANES), F32),
        ],
        compiler_params=grant(2),
        name="smooth_y",
    )(coarse, near, far, coefs)


def interior_kernel(p_ref, s_ref, k_ref, w_ref, m_ref, o_ref, e_ref, hi_ref, lo_ref, f_ref, *, chunks):
    members, _, _, _, owners, _ = p_ref.shape
    tiles = members * owners // LANES
    for n, q in enumerate(chunks):
        for t in range(tiles):
            at = n * tiles + t
            for b in range(CY):
                e_ref[at, b * EXT + 8 : b * EXT + 8 + CX, :] = s_ref[at, b * CX : (b + 1) * CX, :]
            for j in (6, 7, 8 + CX, 9 + CX):
                e_ref[at, pl.ds(j, CY, stride=EXT), :] = jnp.zeros((CY, LANES), F32)
            scale = w_ref[:, t * LANES : (t + 1) * LANES]
            coef = [k_ref[d : d + 1, q * LANES : (q + 1) * LANES] * scale for d in range(5)]
            for b in range(CY):
                acc = coef[0] * e_ref[at, b * EXT + 6 : b * EXT + 6 + CX, :]
                for d in range(1, 5):
                    acc = acc + coef[d] * e_ref[at, b * EXT + 6 + d : b * EXT + 6 + d + CX, :]
                high, low = split_terms(acc)
                hi_ref[n, b * CX : (b + 1) * CX, t * LANES : (t + 1) * LANES] = high
                lo_ref[n, b * CX : (b + 1) * CX, t * LANES : (t + 1) * LANES] = low
        dims = (((0,), (0,)), ((), ()))
        fine = lax.dot_general(hi_ref[n], m_ref[...], dims, preferred_element_type=F32)
        f_ref[n] = fine + lax.dot_general(lo_ref[n], m_ref[...], dims, preferred_element_type=F32)
        for c in range(CB):
            lanes = slice(c * LANES, (c + 1) * LANES)

            def one(k, acc):
                at = pl.ds(k * owners, owners)
                local = f_ref[n, at, lanes]
                return tuple(acc[v] + p_ref[k, v, q, c] * local for v in range(VARS))

            zero = jnp.zeros((owners, LANES), F32)
            acc = lax.fori_loop(0, members, one, (zero,) * VARS, unroll=True)
            for v in range(VARS):
                o_ref[pl.ds((n * VARS + v) * CB + c, owners, stride=len(chunks) * ROWS), :] = acc[v]


def interior(split, smoothed, coefs, scale, matrix, chunks):
    members, _, _, _, owners, _ = split.shape
    return pl.pallas_call(
        functools.partial(interior_kernel, chunks=chunks),
        in_specs=[vmem()] * 5,
        out_specs=vmem(),
        out_shape=jax.ShapeDtypeStruct((owners * len(chunks) * ROWS, LANES), F32),
        scratch_shapes=[
            pltpu.VMEM((smoothed.shape[0], CY * EXT + 8, LANES), F32),
            pltpu.VMEM((len(chunks), CELLS, members * owners), BF16),
            pltpu.VMEM((len(chunks), CELLS, members * owners), BF16),
            pltpu.VMEM((len(chunks), members * owners, COLS), F32),
        ],
        compiler_params=grant(8),
        name="interior",
    )(split, smoothed, coefs, scale, matrix)


def halo_kernel(p_ref, l_ref, near_ref, far_ref, k_ref, w_ref, m_ref, o_ref, hi_ref, lo_ref, f_ref, *, chunks, blocks):
    odd_x = lax.axis_index("tile") // GRID_Y % 2 == 1
    members, _, _, _, owners, _ = p_ref.shape
    tiles = members * owners // LANES
    stride = len(chunks) * ROWS
    o_ref[...] = l_ref[...]
    for n, q in enumerate(chunks):
        for t in range(tiles):
            before, after = sides(near_ref[n * tiles + t], far_ref[n * tiles + t], odd_x)
            scale = w_ref[:, t * LANES : (t + 1) * LANES]
            coef = [k_ref[d : d + 1, q * LANES : (q + 1) * LANES] * scale for d in range(5)]
            cells = [
                coef[0] * before[:CY] + coef[1] * before[CY:],
                coef[0] * before[CY:],
                coef[4] * after[:CY],
                coef[3] * after[:CY] + coef[4] * after[CY:],
            ]
            for e, cell in enumerate(cells):
                high, low = split_terms(cell)
                hi_ref[n, e * CY : (e + 1) * CY, t * LANES : (t + 1) * LANES] = high
                lo_ref[n, e * CY : (e + 1) * CY, t * LANES : (t + 1) * LANES] = low
        dims = (((0,), (0,)), ((), ()))
        fine = lax.dot_general(hi_ref[n], m_ref[...], dims, preferred_element_type=F32)
        f_ref[n] = fine + lax.dot_general(lo_ref[n], m_ref[...], dims, preferred_element_type=F32)
        for i, c in enumerate(blocks):
            acc = [jnp.zeros((owners, LANES), F32)] * VARS
            for k in range(members):
                local = f_ref[n, k * owners : (k + 1) * owners, i * LANES : (i + 1) * LANES]
                acc = [acc[v] + p_ref[k, v, q, c] * local for v in range(VARS)]
            for v in range(VARS):
                at = pl.ds((n * VARS + v) * CB + c, owners, stride=stride)
                o_ref[at, :] = l_ref[at, :] + acc[v]


def halo_part(split, partial, near, far, coefs, scale, edge, chunks):
    members, _, _, _, owners, _ = split.shape
    return pl.pallas_call(
        functools.partial(halo_kernel, chunks=chunks, blocks=edge_matrix()[1]),
        in_specs=[vmem()] * 7,
        out_specs=vmem(),
        out_shape=jax.ShapeDtypeStruct(partial.shape, F32),
        scratch_shapes=[
            pltpu.VMEM((len(chunks), edge.shape[0], members * owners), BF16),
            pltpu.VMEM((len(chunks), edge.shape[0], members * owners), BF16),
            pltpu.VMEM((len(chunks), members * owners, edge.shape[1]), F32),
        ],
        compiler_params=grant(6),
        name="halo_part",
    )(split, partial, near, far, coefs, scale, edge)


def update_kernel(r_ref, *refs, size, last):
    ins, outs = (refs[:3], refs[3:]) if last else (refs[:4], refs[4:])
    rows = ins[0].shape[0]
    total = r_ref[:rows, :]
    for d in range(1, size):
        total = total + r_ref[d * rows : (d + 1) * rows, :]
    if last:
        a_ref, g_ref, sv_ref = ins
        analysis = a_ref[...]
    else:
        g_ref, sv_ref, w_ref, inn_ref = ins
        analysis = jnp.zeros_like(total)
    inc = total + sv_ref[...] * g_ref[...]
    analysis = analysis - 0.5 * (analysis + inc)
    if last:
        own = rows // ROWS
        for q in range(own):
            for v in range(VARS):
                for c in range(CB):
                    row = (q * VARS + v) * CB + c
                    outs[0][v, q : q + 1, c * LANES : (c + 1) * LANES] = analysis[row : row + 1, :]
        return
    grad = w_ref[...] * (analysis - inn_ref[...])
    outs[0][...] = analysis
    outs[1][...] = grad
    for d in range(size):
        outs[2][d * rows : (d + 1) * rows, :] = grad


def update(received, args, size, last):
    rows = received.shape[0] // size
    flat = jax.ShapeDtypeStruct((rows, LANES), F32)
    if last:
        shapes = [jax.ShapeDtypeStruct((VARS, rows // ROWS, COLS), F32)]
    else:
        shapes = [flat, flat, jax.ShapeDtypeStruct((size * rows, LANES), F32)]
    return pl.pallas_call(
        functools.partial(update_kernel, size=size, last=last),
        in_specs=[vmem()] * (1 + len(args)),
        out_specs=[vmem()] * len(shapes),
        out_shape=shapes,
        compiler_params=grant(2),
        name="update",
    )(received, *args)


def exchange(x, size):
    blocks = x.reshape(size, -1, LANES)
    return lax.all_to_all(blocks, "mem", 0, 0, tiled=True).reshape(x.shape)


def swapped(near, far, stride, places, periodic):
    def pairs(is_near):
        out = []
        for i in range(lax.axis_size("tile")):
            place = i // stride % places
            to = place + (1 if (place % 2 == 0) == is_near else -1)
            if periodic or 0 <= to < places:
                out.append((i, i + (to % places - place) * stride))
        return out

    from_far = lax.ppermute(far, "tile", pairs(False))
    from_near = lax.ppermute(near, "tile", pairs(True))
    return from_near, from_far


def body(perturbations, member_weight, innovation, obs_weight, static_var, obs_mask, kernel_x, kernel_y):
    size = lax.axis_size("mem")
    grid_x = lax.axis_size("tile") // GRID_Y
    chunks = tuple(range(perturbations.shape[2] // size))
    split, matrix, edge, innov, static, weight, gradient, to_send, coef_x, coef_y, scale = opening(
        perturbations, innovation, static_var, obs_mask, obs_weight, kernel_x, kernel_y, member_weight, size
    )
    analysis = None
    for step in range(STEPS):
        gathered = exchange(to_send, size)
        coarse, near, far = project(split, gathered, matrix, chunks)
        near, far = swapped(near, far, 1, GRID_Y, False)
        smoothed, near, far = smooth_y(coarse, near, far, coef_y, chunks)
        near, far = swapped(near, far, GRID_Y, grid_x, True)
        partial = interior(split, smoothed, coef_x, scale, matrix, chunks)
        partial = halo_part(split, partial, near, far, coef_x, scale, edge, chunks)
        received = exchange(partial, size)
        if step == STEPS - 1:
            return update(received, (analysis, gradient, static), size, True)[0]
        analysis, gradient, to_send = update(received, (gradient, static, weight, innov), size, False)


def solution(mesh):
    placed = (
        P("mem", None, None, "tile"),
        P("mem"),
        P(None, "mem", "tile"),
        P(None, "mem"),
        P(None, "mem", "tile"),
        P("tile"),
        P(),
        P(),
    )
    return jax.shard_map(
        body, mesh=mesh, in_specs=placed, out_specs=P(None, "mem", "tile"), check_vma=False
    )
```
